512 devices in a mesh: seq: 64 (over y_lo, z, core), clip: 8 (over x, y_hi).
Axes of the slice: x: 4, y: 4 (y_hi: 2, y_lo: 2; y = y_hi * 2 + y_lo), z: 16, core: 2. Of those that a mesh axis runs over, the one named last changes fastest.
Arguments:
- block_input: bfloat16 [8, 64, 128, 1152], P('clip', 'seq'), may hold values from -8 to 8
- out_grad: bfloat16 [8, 64, 128, 1152], P('clip', 'seq'), may hold values from -16 to 16
- spatial_qkv: bfloat16 [8, 64, 128, 3456], P('clip', 'seq'), may hold values from -32 to 32, as said below
- norm_gain: float32 [1152], replicated, may hold values from 0.25 to 1.75
- qkv_weight: bfloat16 [1152, 3456], P('seq'), may hold values from -1 to 1
- qkv_bias: float32 [3456], replicated, may hold values from -3 to 3
- out_weight: bfloat16 [1152, 1152], P('seq'), may hold values from -0.1875 to 0.1875
- spatial_out_weight: bfloat16 [1152, 1152], P('seq'), may hold values from -0.1875 to 0.1875
- grad_sums: float32 [9, 1152], P(None, 'seq'), may hold values from -6 to 6
Outputs:
- resid_grad: bfloat16 [8, 64, 128, 1152], P('clip', 'seq')
- spatial_qkv_grad: bfloat16 [8, 64, 128, 3456], P('clip', 'seq')
- grad_totals: float32 [9, 1152], P(None, 'seq')
The draws below stay inside these ranges and needn't reach their ends.
Inputs may be any that keep to these rules, and one draw needn't show every extreme that they name: `spatial_qkv`: the last dimension holds queries, keys and values in this order, each as 16 heads of 72 entries.
All inputs are finite; a program needn't handle non-finite values.
Results may differ from the reference program's by a relative error of at most 0.012.
The reference program's roundings to bfloat16 on the way count: a program that leaves them out, or rounds other values in their place, can miss the bound.
Values may be sent and summed in bfloat16 or wider, within the bound.
A program may use at most 128 MiB of HBM per device.

```python
import jax
import jax.numpy as jnp
from jax import lax

D = 1152
HEADS = 16
PATCHES = 128
FRAMES = 64
CLIPS = 8


def draw_block_input(key, part):
    full_shape = (CLIPS, FRAMES, PATCHES, D)
    drawn = jnp.clip(jax.random.normal(key, full_shape, jnp.float32), -5.0, 5.0)
    return drawn.astype(jnp.bfloat16)


def draw_spatial_qkv(key, part):
    full_shape = (CLIPS, FRAMES, PATCHES, 3, HEADS, D // HEADS)
    drawn = jnp.clip(jax.random.normal(key, full_shape, jnp.float32), -5.0, 5.0)
    return drawn.reshape(CLIPS, FRAMES, PATCHES, 3 * D).astype(jnp.bfloat16)


def draw_qkv_weight(key, part):
    full_shape = (D, 3, HEADS, D // HEADS)
    drawn = jnp.clip(jax.random.normal(key, full_shape, jnp.float32), -5.0, 5.0) / D ** 0.5
    drawn = jnp.clip(drawn, -1.0, 1.0)
    return drawn.reshape(D, 3 * D).astype(jnp.bfloat16)


def raised(values, rng, source, target, parts, factor):
    def block_of(dim):
        return (jnp.arange(values.shape[dim]) // (values.shape[dim] // parts)).reshape((-1,) + (1,) * (values.ndim - 1 - dim))

    near = jax.random.permutation(rng, parts)[block_of(target)]
    far = (block_of(target) + parts // 2) % parts
    return jnp.where((block_of(source) == near) | (block_of(source) == far), factor * values, values)


def block_scale(stream_key, extent, split, low, largest):
    gain, own = 1.0, jax.random.fold_in(stream_key, 6)
    for dim, parts in split:
        steps = jnp.exp(jax.random.uniform(jax.random.fold_in(own, dim), (parts,), jnp.float32, low / len(split), largest / len(split)))
        gain = gain * jnp.repeat(steps, extent[dim] // parts).reshape([-1 if axis == dim else 1 for axis in range(len(extent))])
    return gain


def gaussian(stream_key, shape, scale, bound, cuts=(), kind=jnp.bfloat16):
    values = jax.random.normal(stream_key, shape, jnp.float32) * scale
    if len(cuts) > 0:
        values = block_scale(stream_key, shape, cuts, -0.22, 0.18) * values
    return jnp.clip(values, min=-bound, max=bound).astype(kind)


def bell_draw_with(key, shape, width, reach, shards, heavy, dtype=jnp.bfloat16):
    values = width * jax.random.normal(key, shape, jnp.float32)
    if shards:
        values = values * block_scale(key, shape, shards, -0.22, 0.18)
    return jnp.clip(raised(values, jax.random.fold_in(key, 3), *heavy), -reach, reach).astype(dtype)


def setup_inputs(seed: int = 0) -> dict:
    splits = jax.random.split(jax.random.key(seed), 10)
    return {
        "block_input": draw_block_input(jax.random.fold_in(splits[9], 71), 0),
        "out_grad": bell_draw_with(splits[1], (CLIPS, FRAMES, PATCHES, D), 1.0, 16.0, ((0, 8), (1, 64)), (1, 3, 64, 4.0)),
        "spatial_qkv": draw_spatial_qkv(jax.random.fold_in(splits[9], 71), 0),
        "norm_gain": jnp.clip(1.0 + 0.15 * jax.random.normal(splits[3], (D,), jnp.float32), 0.25, 1.75),
        "qkv_weight": draw_qkv_weight(jax.random.fold_in(splits[9], 71), 0),
        "qkv_bias": gaussian(splits[5], (3 * D,), 0.5, 3.0, (), jnp.float32),
        "out_weight": gaussian(splits[6], (D, D), D ** -0.5, 0.1875, ((0, 64),)),
        "spatial_out_weight": gaussian(splits[7], (D, D), D ** -0.5, 0.1875, ((0, 64),)),
        "grad_sums": gaussian(splits[8], (9, D), 1.0, 6.0, ((1, 64),), jnp.float32),
    }


EPS = 1e-06
HIGHEST = lax.Precision.HIGHEST

def rounded(values):
    return lax.optimization_barrier(values.astype(jnp.bfloat16)).astype(jnp.float32)

def attention_back(queries, key_side, value_side, grad_out, layout, factor):
    key_layout = layout.replace('l', 'm')
    queries = queries.astype(jnp.float32)
    key_side = key_side.astype(jnp.float32)
    value_side = value_side.astype(jnp.float32)
    grad_out = grad_out.astype(jnp.float32)
    scores = jnp.einsum(layout + ',' + key_layout + '->bhlm', queries, key_side, precision=HIGHEST) * factor
    weights = jax.nn.softmax(scores, axis=-1)
    grad_value = jnp.einsum('bhlm,' + layout + '->' + key_layout, rounded(weights), grad_out, precision=HIGHEST).astype(jnp.bfloat16)
    grad_weight = jnp.einsum(layout + ',' + key_layout + '->bhlm', grad_out, value_side, precision=HIGHEST)
    grad_score = rounded(weights * (grad_weight - lax.optimization_barrier(jnp.sum(weights * grad_weight, axis=-1, keepdims=True))) * factor)
    grad_query = jnp.einsum('bhlm,' + key_layout + '->' + layout, grad_score, key_side, precision=HIGHEST).astype(jnp.bfloat16)
    grad_key = jnp.einsum('bhlm,' + layout + '->' + key_layout, grad_score, queries, precision=HIGHEST).astype(jnp.bfloat16)
    return (grad_query, grad_key, grad_value)

def one_clip(block_input, out_grad, spatial_qkv, norm_gain, qkv_weight, qkv_bias, out_weight, spatial_out_weight):
    head_dim = D // HEADS
    factor = 1.0 / head_dim ** 0.5
    rows_in = block_input.reshape(FRAMES * PATCHES, D).astype(jnp.float32)
    centred = rows_in - lax.optimization_barrier(jnp.mean(rows_in, axis=-1, keepdims=True))
    inv_std = lax.rsqrt(lax.optimization_barrier(jnp.mean(centred * centred, axis=-1, keepdims=True)) + EPS)
    normal_rows = centred * inv_std
    normed = (normal_rows * norm_gain).astype(jnp.bfloat16)
    qkv_rows = (jnp.dot(normed, qkv_weight, preferred_element_type=jnp.float32) + qkv_bias).astype(jnp.bfloat16)
    qkv_heads = qkv_rows.reshape(FRAMES, PATCHES, 3, HEADS, head_dim)
    grad_rows = out_grad.reshape(FRAMES * PATCHES, D)
    grad_attn = jnp.dot(grad_rows, out_weight.T, preferred_element_type=jnp.float32).astype(jnp.bfloat16)
    grad_query, grad_key, grad_value = attention_back(qkv_heads[:, :, 0], qkv_heads[:, :, 1], qkv_heads[:, :, 2], grad_attn.reshape(FRAMES, PATCHES, HEADS, head_dim), 'lbhe', factor)
    grad_qkv = jnp.stack([grad_query, grad_key, grad_value], axis=2).reshape(FRAMES * PATCHES, 3 * D)
    grad_normed = jnp.dot(grad_qkv, qkv_weight.T, preferred_element_type=jnp.float32)
    grad_hat = grad_normed * norm_gain
    branch = inv_std * (grad_hat - lax.optimization_barrier(jnp.mean(grad_hat, axis=-1, keepdims=True)) - normal_rows * lax.optimization_barrier(jnp.mean(grad_hat * normal_rows, axis=-1, keepdims=True)))
    branch = branch.astype(jnp.bfloat16)
    resid_grad = (grad_rows.astype(jnp.float32) + branch.astype(jnp.float32)).astype(jnp.bfloat16)
    grad_sattn = jnp.dot(resid_grad, spatial_out_weight.T, preferred_element_type=jnp.float32).astype(jnp.bfloat16)
    spatial_heads = spatial_qkv.reshape(FRAMES, PATCHES, 3, HEADS, head_dim)
    spatial_query, spatial_key, spatial_value = attention_back(spatial_heads[:, :, 0], spatial_heads[:, :, 1], spatial_heads[:, :, 2], grad_sattn.reshape(FRAMES, PATCHES, HEADS, head_dim), 'blhe', factor)
    spatial_grad = jnp.stack([spatial_query, spatial_key, spatial_value], axis=2).reshape(FRAMES * PATCHES, 3 * D)
    stat_rows = jnp.concatenate([lax.optimization_barrier(jnp.sum(grad_normed * normal_rows, axis=0))[None], lax.optimization_barrier(jnp.sum(grad_qkv.astype(jnp.float32), axis=0)).reshape(3, D), lax.optimization_barrier(jnp.sum(grad_rows.astype(jnp.float32), axis=0))[None], lax.optimization_barrier(jnp.sum(spatial_grad.astype(jnp.float32), axis=0)).reshape(3, D), lax.optimization_barrier(jnp.sum(resid_grad.astype(jnp.float32), axis=0))[None]], axis=0)
    return (resid_grad.reshape(FRAMES, PATCHES, D), spatial_grad.reshape(FRAMES, PATCHES, 3 * D), stat_rows)

def reference(block_input, out_grad, spatial_qkv, norm_gain, qkv_weight, qkv_bias, out_weight, spatial_out_weight, grad_sums):

    def per_clip(members):
        return one_clip(members[0], members[1], members[2], norm_gain, qkv_weight, qkv_bias, out_weight, spatial_out_weight)
    resid_grad, spatial_grad, stat_rows = lax.map(per_clip, (block_input, out_grad, spatial_qkv))
    grad_scale = 1.0 / (CLIPS * FRAMES * PATCHES) ** 0.5
    return (resid_grad, spatial_grad, grad_sums + lax.optimization_barrier(jnp.sum(stat_rows, axis=0)) * grad_scale)
```

```python
import functools
import math

import jax
import jax.numpy as jnp
from jax import lax
from jax.experimental import pallas as pl
from jax.experimental.pallas import tpu as pltpu
from jax.sharding import PartitionSpec as P

HEADS = 16
EPS = 1e-06
MESH = pl.DeviceIdType.MESH
F32 = jnp.float32
BF16 = jnp.bfloat16

D = 1152
CH = 384
NCH = 16
NZ = 16
UNIT = 144
HALF = ((0, 80), (80, 64))


def dev(x, y, z, c):
    return {"clip": x * 2 + y // 2, "seq": (y % 2) * 32 + z * 2 + c}


def place():
    s, q = lax.axis_index("seq"), lax.axis_index("clip")
    x = q // 2
    y = (q % 2) * 2 + s // 32
    z = (s // 2) % 16
    c = s % 2
    return x, y, z, c


def gather_kernel(
    ws, xg, w_out, r_out, zbuf, wbuf, own, loc, swap_s, swap_r, zsend, zrecv, a_send, a_recv,
    p_send, p_recv, d_send, d_recv, h_sem,
):
    x, y, z, c = place()
    s, q = lax.axis_index("seq"), lax.axis_index("clip")
    ylo = s // 32
    sib = dev(x, y, z, 1 - c)

    def near(axis, step):
        if axis == 0:
            return (x + step + 4) % 4, y
        return x, (y + step + 4) % 4

    barrier = pltpu.get_barrier_semaphore()
    partners = [
        sib,
        dev(x, y, (z + 1) % NZ, c),
        dev(x, y, (z + NZ - 1) % NZ, c),
        dev(x, y, (z + 2) % NZ, c),
        dev(x, y, (z + NZ - 2) % NZ, c),
        dev(*near(0, 1), z, c),
        dev(*near(0, -1), z, c),
        dev(*near(1, 1), z, c),
        dev(*near(1, -1), z, c),
        {"clip": q, "seq": (1 - ylo) * 32 + z * 2 + 1 - c},
    ]
    for p in partners:
        pl.semaphore_signal(barrier, inc=1, device_id=p, device_id_type=MESH)
    pl.semaphore_wait(barrier, len(partners))

    keep = pltpu.make_async_copy(ws.at[2 * q + c], zbuf.at[z, c], loc.at[0])
    keep.start()
    swap = pltpu.make_async_remote_copy(
        ws.at[2 * q + 1 - c], zbuf.at[z, c], swap_s, swap_r, device_id=sib, device_id_type=MESH
    )
    swap.start()
    mine = pltpu.make_async_copy(xg.at[s], own, loc.at[1])
    mine.start()
    keep.wait()
    pltpu.make_async_remote_copy(
        ws.at[2 * q + 1 - c], zbuf.at[z, 1 - c], swap_s, swap_r, device_id=sib, device_id_type=MESH
    ).wait_recv()
    mine.wait()
    put = pltpu.make_async_copy(own, r_out.at[s], loc.at[2])
    put.start()

    def zcopy(origin, step):
        o = (origin + 2 * NZ) % NZ
        return pltpu.make_async_remote_copy(
            zbuf.at[o], zbuf.at[o], zsend, zrecv.at[o],
            device_id=dev(x, y, (z + step + NZ) % NZ, c), device_id_type=MESH,
        )

    def zwait(origin):
        zcopy(origin, 1).wait_recv()

    def a2a(dist, count=4):
        zz = (z + dist + NZ) % NZ

        def one(i, carry):
            t = (i // 2) * 32 + zz * 2 + i % 2
            pltpu.make_async_remote_copy(
                xg.at[t], r_out.at[s], a_send, a_recv,
                device_id={"clip": q, "seq": t}, device_id_type=MESH,
            ).start()
            return carry

        lax.fori_loop(0, 4, one, 0)

    def a2a_home():
        for yl, cc in ((ylo, 1 - c), (1 - ylo, c), (1 - ylo, 1 - c)):
            t = yl * 32 + z * 2 + cc
            pltpu.make_async_remote_copy(
                xg.at[t], r_out.at[s], a_send, a_recv,
                device_id={"clip": q, "seq": t}, device_id_type=MESH,
            ).start()

    group = z // 4
    order = [group, (group + 1) % 4, (group + 3) % 4, (group + 2) % 4]

    def spot(u, h, xx, yy):
        off, n = HALF[h]
        at = (xx * 2 + yy // 2) * D + (yy % 2) * 576 + order[u] * UNIT + off
        return pl.multiple_of(at, 16), n

    def push(u, h, xx, yy, axis, step):
        at, n = spot(u, h, xx, yy)
        nx, ny = near(axis, step)
        pltpu.make_async_remote_copy(
            wbuf.at[pl.ds(at, n)], wbuf.at[pl.ds(at, n)], p_send,
            p_recv.at[(u * 2 + h) * 16 + xx * 4 + yy],
            device_id=dev(nx, ny, z, c), device_id_type=MESH,
        ).start()

    def deliver(u, h, xx, yy):
        at, n = spot(u, h, xx, yy)
        to = pl.multiple_of(at + (xx * 2 + yy // 2) * D + c * D, 16)
        pltpu.make_async_remote_copy(
            wbuf.at[pl.ds(at, n)], w_out.at[pl.ds(to, n)], d_send, d_recv,
            device_id=sib, device_id_type=MESH,
        ).start()
        pltpu.make_async_copy(wbuf.at[pl.ds(at, n)], w_out.at[pl.ds(to, n)], h_sem).start()

    def arrive(u, h, xx, yy):
        at, n = spot(u, h, xx, yy)
        pltpu.make_async_remote_copy(
            wbuf.at[pl.ds(at, n)], wbuf.at[pl.ds(at, n)], p_send,
            p_recv.at[(u * 2 + h) * 16 + xx * 4 + yy],
            device_id=sib, device_id_type=MESH,
        ).wait_recv()
        deliver(u, h, xx, yy)

    def cell(axis, a, b):
        if axis == 0:
            return (x + a + 4) % 4, (y + b + 4) % 4
        return (x + b + 4) % 4, (y + a + 4) % 4

    def ways(u, h):
        first = (u + h) % 2
        return first, 1 - first, (1 if (u // 2 + h) % 2 == 0 else -1)

    def launch(u):
        for t in range(3):
            parts = []
            for zi in range(4):
                for cc in range(2):
                    parts.append(zbuf[order[u] * 4 + zi, cc, 18 * t : 18 * t + 18, :].astype(F32))
            at, _ = spot(u, 0, x, y)
            wbuf[pl.ds(at, UNIT), 128 * t : 128 * t + 128] = jnp.concatenate(parts, axis=0).astype(BF16)
        for h in range(2):
            first, second, _ = ways(u, h)
            for step in (1, -1):
                push(u, h, x, y, first, step)
            for step in (1, -1):
                push(u, h, x, y, second, step)
            deliver(u, h, x, y)

    def round_one(u):
        for h in range(2):
            first, second, f = ways(u, h)
            for a in (-f, f):
                blk = cell(first, a, 0)
                arrive(u, h, *blk)
                if a == -f:
                    push(u, h, *blk, first, f)
                for step in (1, -1):
                    push(u, h, *blk, second, step)
            for b in (-f, f):
                blk = cell(first, 0, b)
                arrive(u, h, *blk)
                if b == -f:
                    push(u, h, *blk, second, f)

    def round_two(u):
        for h in range(2):
            first, second, f = ways(u, h)
            blk = cell(first, 2, 0)
            arrive(u, h, *blk)
            for step in (1, -1):
                push(u, h, *blk, second, step)
            for a in (-f, f):
                for b in (-f, f):
                    blk = cell(first, a, b)
                    arrive(u, h, *blk)
                    if b == -f:
                        push(u, h, *blk, second, f)

    def round_three(u):
        for h in range(2):
            first, second, f = ways(u, h)
            arrive(u, h, *cell(first, 0, 2))
            for b in (-f, f):
                blk = cell(first, 2, b)
                arrive(u, h, *blk)
                if b == -f:
                    push(u, h, *blk, second, f)
            for a in (-f, f):
                arrive(u, h, *cell(first, a, 2))

    def round_four(u):
        for h in range(2):
            first, _, _ = ways(u, h)
            arrive(u, h, *cell(first, 2, 2))

    for step in (1, -1, 2, -2):
        zcopy(z, step).start()
    for k in (1, 2, 3):
        for d in (2 * k - 1, 2 * k):
            zwait(z - d)
            zwait(z + d)
        zcopy(z - 2 * k, 1).start()
        zcopy(z + 2 * k, -1).start()
        zcopy(z - 2 * k, 2).start()
        if k < 3:
            zcopy(z + 2 * k, -2).start()
        if k == 1:
            a2a_home()
        for d in (2 * k - 1, 2 * k):
            a2a(d)
            a2a(-d)
        if k == 2:
            launch(0)
        if k == 3:
            round_one(0)
    zwait(z - 7)
    zwait(z + 7)
    zwait(z - 8)
    a2a(7)
    a2a(-7)
    a2a(8)
    launch(1)
    launch(2)
    round_two(0)
    launch(3)
    round_one(1)
    round_one(2)
    round_three(0)
    round_one(3)
    round_two(1)
    round_two(2)
    round_four(0)
    round_two(3)
    round_three(1)
    round_three(2)
    round_three(3)
    round_four(1)
    round_four(2)
    round_four(3)

    swap.wait_send()
    put.wait()
    pltpu.make_async_copy(xg.at[pl.ds(0, 63)], xg.at[pl.ds(0, 63)], a_send).wait()
    pltpu.make_async_copy(r_out.at[pl.ds(0, 63)], r_out.at[pl.ds(0, 63)], a_recv).wait()
    pltpu.make_async_copy(zbuf.at[pl.ds(0, 15)], zbuf.at[pl.ds(0, 15)], zsend).wait()
    sent = wbuf.at[pl.ds(0, 60 * UNIT)]
    pltpu.make_async_copy(sent, sent, p_send).wait()
    pltpu.make_async_copy(wbuf, wbuf, d_send).wait()
    half = w_out.at[pl.ds(0, 8 * D)]
    pltpu.make_async_copy(half, half, d_recv).wait()
    pltpu.make_async_copy(wbuf, half, h_sem).wait()


def gather_all(ws, xg):
    dma = pltpu.SemaphoreType.DMA
    return pl.pallas_call(
        gather_kernel,
        out_shape=(
            jax.ShapeDtypeStruct((NCH * D, CH), BF16),
            jax.ShapeDtypeStruct((64, 4, D), BF16),
        ),
        in_specs=[pl.BlockSpec(memory_space=pl.ANY)] * 2,
        out_specs=(pl.BlockSpec(memory_space=pl.ANY),) * 2,
        scratch_shapes=[
            pltpu.VMEM((NZ, 2, 54, 128), BF16),
            pltpu.VMEM((8 * D, CH), BF16),
            pltpu.VMEM((4, D), BF16),
            dma((3,)), dma, dma, dma, dma((NZ,)), dma, dma,
            dma, dma((128,)), dma, dma, dma,
        ],
        compiler_params=pltpu.CompilerParams(
            collective_id=0, has_side_effects=True, vmem_limit_bytes=40 << 20
        ),
        name="gather_all",
    )(ws, xg)


NT = (((1,), (1,)), ((), ()))
TN = (((0,), (0,)), ((), ()))
NN = (((1,), (0,)), ((), ()))


def mm(a, b, dims):
    return lax.dot_general(a, b, dims, preferred_element_type=F32)


def head_back(qh, kh, vh, gh, factor, mask):
    scores = mm(qh, kh, NT) * factor
    if mask is not None:
        scores = jnp.where(mask, scores, -jnp.inf)
    top = jnp.max(scores, axis=-1, keepdims=True)
    e = jnp.exp(scores - top)
    weights = e / jnp.sum(e, axis=-1, keepdims=True)
    grad_value = mm(weights.astype(BF16), gh, TN)
    grad_weight = mm(gh, vh, NT)
    r = jnp.sum(weights * grad_weight, axis=-1, keepdims=True)
    gs = (weights * (grad_weight - r) * factor).astype(BF16)
    grad_query = mm(gs, kh, NN)
    grad_key = mm(gs, qh, TN)
    return grad_query.astype(BF16), grad_key.astype(BF16), grad_value.astype(BF16)


def temporal_kernel(
    r_ref, w_hbm, gain_ref, bias_ref, branch_ref, sums_ref, wv, qkv_s, g_s, ga_s, dq_s, sems,
):
    head_dim = D // HEADS
    factor = 1.0 / math.sqrt(head_dim)
    copies = []
    for j in range(12):
        cp = pltpu.make_async_copy(w_hbm.at[pl.ds(j * D, D)], wv.at[pl.ds(j * D, D)], sems.at[j])
        cp.start()
        copies.append(cp)
    rows = r_ref[...].astype(F32)
    xr = rows[:, 0:2, :].reshape(128, D)
    g = rows[:, 2:4, :].reshape(128, D)
    sums_ref[4:5, :] = jnp.sum(g, axis=0, keepdims=True)
    g_s[...] = g.astype(BF16)
    mean = jnp.mean(xr, axis=-1, keepdims=True)
    centred = xr - mean
    inv_std = lax.rsqrt(jnp.mean(centred * centred, axis=-1, keepdims=True) + EPS)
    normal = centred * inv_std
    gain = gain_ref[...]
    normed = (normal * gain).astype(BF16)
    for j in range(9):
        copies[j].wait()
        qkv_s[:, CH * j : CH * j + CH] = (
            mm(normed, wv[j * D : j * D + D, :], NN) + bias_ref[:, CH * j : CH * j + CH]
        ).astype(BF16)
    acc = None
    for j in range(3):
        copies[9 + j].wait()
        part = mm(g_s[:, CH * j : CH * j + CH], wv[(9 + j) * D : (10 + j) * D, :], NT)
        acc = part if acc is None else acc + part
    ga_s[...] = acc.astype(BF16)
    ri = lax.broadcasted_iota(jnp.int32, (128, 128), 0)
    ci = lax.broadcasted_iota(jnp.int32, (128, 128), 1)
    mask = (ri & 1) == (ci & 1)
    for h in range(HEADS):
        lo, hi = h * head_dim, (h + 1) * head_dim
        gq, gk, gv = head_back(
            qkv_s[:, lo:hi], qkv_s[:, D + lo : D + hi], qkv_s[:, 2 * D + lo : 2 * D + hi],
            ga_s[:, lo:hi], factor, mask,
        )
        dq_s[:, lo:hi] = gq
        dq_s[:, D + lo : D + hi] = gk
        dq_s[:, 2 * D + lo : 2 * D + hi] = gv
    acc = None
    for j in range(9):
        part = mm(dq_s[:, CH * j : CH * j + CH], wv[j * D : j * D + D, :], NT)
        acc = part if acc is None else acc + part
    grad_normed = acc
    sums_ref[0:1, :] = jnp.sum(grad_normed * normal, axis=0, keepdims=True)
    for j in range(3):
        sums_ref[1 + j : 2 + j, :] = jnp.sum(
            dq_s[:, D * j : D * j + D].astype(F32), axis=0, keepdims=True
        )
    hat = grad_normed * gain
    branch = inv_std * (
        hat
        - jnp.mean(hat, axis=-1, keepdims=True)
        - normal * jnp.mean(hat * normal, axis=-1, keepdims=True)
    )
    branch_ref[...] = branch.reshape(64, 2, D).astype(BF16)


def temporal(r, w, gain, bias):
    vm = pl.BlockSpec(memory_space=pltpu.VMEM)
    return pl.pallas_call(
        temporal_kernel,
        out_shape=(
            jax.ShapeDtypeStruct((64, 2, D), BF16),
            jax.ShapeDtypeStruct((5, D), F32),
        ),
        in_specs=[vm, pl.BlockSpec(memory_space=pl.ANY), vm, vm],
        out_specs=(vm, vm),
        scratch_shapes=[
            pltpu.VMEM((12 * D, CH), BF16),
            pltpu.VMEM((128, 3 * D), BF16),
            pltpu.VMEM((128, D), BF16),
            pltpu.VMEM((128, D), BF16),
            pltpu.VMEM((128, 3 * D), BF16),
            pltpu.SemaphoreType.DMA((12,)),
        ],
        compiler_params=pltpu.CompilerParams(vmem_limit_bytes=48 << 20),
        name="temporal",
    )(r, w, gain, bias)


def spatial_kernel(b_ref, g_ref, qkv_ref, w_hbm, resid_ref, dqkv_ref, sums_ref, wv, ga_s, sems):
    head_dim = D // HEADS
    factor = 1.0 / math.sqrt(head_dim)
    copies = []
    for j in range(3):
        cp = pltpu.make_async_copy(
            w_hbm.at[pl.ds((12 + j) * D, D)], wv.at[pl.ds(j * D, D)], sems.at[j]
        )
        cp.start()
        copies.append(cp)
    branch = b_ref[...].astype(F32).reshape(128, D)
    resid = (g_ref[...].astype(F32) + branch).astype(BF16)
    resid_ref[...] = resid
    sums_ref[3:4, :] = jnp.sum(resid.astype(F32), axis=0, keepdims=True)
    acc = None
    for j in range(3):
        copies[j].wait()
        part = mm(resid_ref[:, CH * j : CH * j + CH], wv[j * D : j * D + D, :], NT)
        acc = part if acc is None else acc + part
    ga_s[...] = acc.astype(BF16)
    for h in range(HEADS):
        lo, hi = h * head_dim, (h + 1) * head_dim
        gq, gk, gv = head_back(
            qkv_ref[:, lo:hi], qkv_ref[:, D + lo : D + hi], qkv_ref[:, 2 * D + lo : 2 * D + hi],
            ga_s[:, lo:hi], factor, None,
        )
        dqkv_ref[:, lo:hi] = gq
        dqkv_ref[:, D + lo : D + hi] = gk
        dqkv_ref[:, 2 * D + lo : 2 * D + hi] = gv
    for j in range(3):
        sums_ref[j : j + 1, :] = jnp.sum(
            dqkv_ref[:, D * j : D * j + D].astype(F32), axis=0, keepdims=True
        )


def spatial(b, g, qkv, w):
    vm = pl.BlockSpec(memory_space=pltpu.VMEM)
    return pl.pallas_call(
        spatial_kernel,
        out_shape=(
            jax.ShapeDtypeStruct((128, D), BF16),
            jax.ShapeDtypeStruct((128, 3 * D), BF16),
            jax.ShapeDtypeStruct((4, D), F32),
        ),
        in_specs=[vm, vm, vm, pl.BlockSpec(memory_space=pl.ANY)],
        out_specs=(vm, vm, vm),
        scratch_shapes=[
            pltpu.VMEM((3 * D, CH), BF16),
            pltpu.VMEM((128, D), BF16),
            pltpu.SemaphoreType.DMA((3,)),
        ],
        compiler_params=pltpu.CompilerParams(vmem_limit_bytes=40 << 20),
        name="spatial",
    )(b, g, qkv, w)


def prepare(block_input, out_grad, qkv_weight, out_weight, spatial_out_weight):
    rows = qkv_weight.shape[0]
    pad = jnp.zeros((rows, CH), BF16)
    w = jnp.concatenate([qkv_weight, out_weight, spatial_out_weight, pad], axis=1)
    ws = w.reshape(rows, NCH, 3, 128).transpose(1, 2, 0, 3).reshape(NCH, 3 * rows, 128)
    xg = jnp.concatenate([block_input.reshape(64, 2, D), out_grad.reshape(64, 2, D)], axis=1)
    return ws, xg


def per_device(
    block_input, out_grad, spatial_qkv, norm_gain, qkv_weight, qkv_bias, out_weight,
    spatial_out_weight, grad_sums,
):
    ws, xg = prepare(block_input, out_grad, qkv_weight, out_weight, spatial_out_weight)
    w, r = gather_all(ws, xg)
    branch, sums_a = temporal(r, w, norm_gain.reshape(1, D), qkv_bias.reshape(1, 3 * D))
    back = lax.all_to_all(branch, "seq", split_axis=0, concat_axis=0, tiled=True)
    resid, sgrad, sums_b = spatial(back, out_grad.reshape(128, D), spatial_qkv.reshape(128, 3 * D), w)
    partial_sums = jnp.concatenate([sums_a, sums_b], axis=0)
    n = lax.axis_size("seq")
    blocks = jnp.moveaxis(partial_sums.reshape(9, n, D // n), 1, 0)
    share = jnp.sum(lax.all_to_all(blocks, "seq", 0, 0, tiled=True), axis=0)
    everyone = jnp.broadcast_to(share, (lax.axis_size("clip"), *share.shape))
    total = jnp.sum(lax.all_to_all(everyone, "clip", 0, 0, tiled=True), axis=0)
    tokens = 128 * lax.axis_size("seq") * lax.axis_size("clip")
    return (
        resid.reshape(1, 1, 128, D),
        sgrad.reshape(1, 1, 128, 3 * D),
        grad_sums + total * (1.0 / math.sqrt(tokens)),
    )


def solution(mesh):
    in_specs = (
        P("clip", "seq", None, None),
        P("clip", "seq", None, None),
        P("clip", "seq", None, None),
        P(),
        P("seq", None),
        P(),
        P("seq", None),
        P("seq", None),
        P(None, "seq"),
    )
    out_specs = (P("clip", "seq", None, None), P("clip", "seq", None, None), P(None, "seq"))
    return jax.shard_map(
        per_device, mesh=mesh, in_specs=in_specs, out_specs=out_specs, check_vma=False
    )
```

```python
import functools
import math

import jax
import jax.numpy as jnp
from jax import lax
from jax.experimental import pallas as pl
from jax.experimental.pallas import tpu as pltpu
from jax.sharding import PartitionSpec as P

HEADS = 16
EPS = 1e-06
MESH = pl.DeviceIdType.MESH
F32 = jnp.float32
BF16 = jnp.bfloat16

D = 1152
CH = 384
NCH = 16
NZ = 16
UNIT = 144
HALF = ((0, 80), (80, 64))


def dev(x, y, z, c):
    return {"clip": x * 2 + y // 2, "seq": (y % 2) * 32 + z * 2 + c}


def place():
    s, q = lax.axis_index("seq"), lax.axis_index("clip")
    x = q // 2
    y = (q % 2) * 2 + s // 32
    z = (s // 2) % 16
    c = s % 2
    return x, y, z, c


def gather_kernel(
    ws, xg, w_out, r_out, zbuf, wbuf, own, loc, swap_s, swap_r, zsend, zrecv, a_send, a_recv,
    p_send, p_recv, d_send, d_recv, h_sem,
):
    x, y, z, c = place()
    s, q = lax.axis_index("seq"), lax.axis_index("clip")
    ylo = s // 32
    sib = dev(x, y, z, 1 - c)

    def near(axis, step):
        if axis == 0:
            return (x + step + 4) % 4, y
        return x, (y + step + 4) % 4

    barrier = pltpu.get_barrier_semaphore()
    partners = [
        sib,
        dev(x, y, (z + 1) % NZ, c),
        dev(x, y, (z + NZ - 1) % NZ, c),
        dev(x, y, (z + 2) % NZ, c),
        dev(x, y, (z + NZ - 2) % NZ, c),
        dev(*near(0, 1), z, c),
        dev(*near(0, -1), z, c),
        dev(*near(1, 1), z, c),
        dev(*near(1, -1), z, c),
        {"clip": q, "seq": (1 - ylo) * 32 + z * 2 + 1 - c},
    ]
    for p in partners:
        pl.semaphore_signal(barrier, inc=1, device_id=p, device_id_type=MESH)
    pl.semaphore_wait(barrier, len(partners))

    keep = pltpu.make_async_copy(ws.at[2 * q + c], zbuf.at[z, c], loc.at[0])
    keep.start()
    swap = pltpu.make_async_remote_copy(
        ws.at[2 * q + 1 - c], zbuf.at[z, c], swap_s, swap_r, device_id=sib, device_id_type=MESH
    )
    swap.start()
    mine = pltpu.make_async_copy(xg.at[s], own, loc.at[1])
    mine.start()
    keep.wait()
    pltpu.make_async_remote_copy(
        ws.at[2 * q + 1 - c], zbuf.at[z, 1 - c], swap_s, swap_r, device_id=sib, device_id_type=MESH
    ).wait_recv()
    mine.wait()
    put = pltpu.make_async_copy(own, r_out.at[s], loc.at[2])
    put.start()

    def zcopy(origin, step):
        o = (origin + 2 * NZ) % NZ
        return pltpu.make_async_remote_copy(
            zbuf.at[o], zbuf.at[o], zsend, zrecv.at[o],
            device_id=dev(x, y, (z + step + NZ) % NZ, c), device_id_type=MESH,
        )

    def zwait(origin):
        zcopy(origin, 1).wait_recv()

    def a2a(dist, count=4):
        zz = (z + dist + NZ) % NZ

        def one(i, carry):
            t = (i // 2) * 32 + zz * 2 + i % 2
            pltpu.make_async_remote_copy(
                xg.at[t], r_out.at[s], a_send, a_recv,
                device_id={"clip": q, "seq": t}, device_id_type=MESH,
            ).start()
            return carry

        lax.fori_loop(0, 4, one, 0)

    def a2a_home():
        for yl, cc in ((ylo, 1 - c), (1 - ylo, c), (1 - ylo, 1 - c)):
            t = yl * 32 + z * 2 + cc
            pltpu.make_async_remote_copy(
                xg.at[t], r_out.at[s], a_send, a_recv,
                device_id={"clip": q, "seq": t}, device_id_type=MESH,
            ).start()

    group = z // 4
    order = [group, (group + 1) % 4, (group + 3) % 4, (group + 2) % 4]

    def spot(u, h, xx, yy):
        off, n = HALF[h]
        at = (xx * 2 + yy // 2) * D + (yy % 2) * 576 + order[u] * UNIT + off
        return pl.multiple_of(at, 16), n

    def push(u, h, xx, yy, axis, step):
        at, n = spot(u, h, xx, yy)
        nx, ny = near(axis, step)
        pltpu.make_async_remote_copy(
            wbuf.at[pl.ds(at, n)], wbuf.at[pl.ds(at, n)], p_send,
            p_recv.at[(u * 2 + h) * 16 + xx * 4 + yy],
            device_id=dev(nx, ny, z, c), device_id_type=MESH,
        ).start()

    def deliver(u, h, xx, yy):
        at, n = spot(u, h, xx, yy)
        to = pl.multiple_of(at + (xx * 2 + yy // 2) * D + c * D, 16)
        pltpu.make_async_remote_copy(
            wbuf.at[pl.ds(at, n)], w_out.at[pl.ds(to, n)], d_send, d_recv,
            device_id=sib, device_id_type=MESH,
        ).start()
        pltpu.make_async_copy(wbuf.at[pl.ds(at, n)], w_out.at[pl.ds(to, n)], h_sem).start()

    def arrive(u, h, xx, yy):
        at, n = spot(u, h, xx, yy)
        pltpu.make_async_remote_copy(
            wbuf.at[pl.ds(at, n)], wbuf.at[pl.ds(at, n)], p_send,
            p_recv.at[(u * 2 + h) * 16 + xx * 4 + yy],
            device_id=sib, device_id_type=MESH,
        ).wait_recv()
        deliver(u, h, xx, yy)

    def cell(axis, a, b):
        if axis == 0:
            return (x + a + 4) % 4, (y + b + 4) % 4
        return (x + b + 4) % 4, (y + a + 4) % 4

    def ways(u, h):
        first = (u + h) % 2
        return first, 1 - first, (1 if (u // 2 + h) % 2 == 0 else -1)

    def launch(u):
        for t in range(3):
            parts = []
            for zi in range(4):
                for cc in range(2):
                    parts.append(zbuf[order[u] * 4 + zi, cc, 18 * t : 18 * t + 18, :].astype(F32))
            at, _ = spot(u, 0, x, y)
            wbuf[pl.ds(at, UNIT), 128 * t : 128 * t + 128] = jnp.concatenate(parts, axis=0).astype(BF16)
        for h in range(2):
            first, second, _ = ways(u, h)
            for step in (1, -1):
                push(u, h, x, y, first, step)
            for step in (1, -1):
                push(u, h, x, y, second, step)
            deliver(u, h, x, y)

    def round_one(u):
        for h in range(2):
            first, second, f = ways(u, h)
            for a in (-f, f):
                blk = cell(first, a, 0)
                arrive(u, h, *blk)
                if a == -f:
                    push(u, h, *blk, first, f)
                for step in (1, -1):
                    push(u, h, *blk, second, step)
            for b in (-f, f):
                blk = cell(first, 0, b)
                arrive(u, h, *blk)
                if b == -f:
                    push(u, h, *blk, second, f)

    def round_two(u):
        for h in range(2):
            first, second, f = ways(u, h)
            blk = cell(first, 2, 0)
            arrive(u, h, *blk)
            for step in (1, -1):
                push(u, h, *blk, second, step)
            for a in (-f, f):
                for b in (-f, f):
                    blk = cell(first, a, b)
                    arrive(u, h, *blk)
                    if b == -f:
                        push(u, h, *blk, second, f)

    def round_three(u):
        for h in range(2):
            first, second, f = ways(u, h)
            arrive(u, h, *cell(first, 0, 2))
            for b in (-f, f):
                blk = cell(first, 2, b)
                arrive(u, h, *blk)
                if b == -f:
                    push(u, h, *blk, second, f)
            for a in (-f, f):
                arrive(u, h, *cell(first, a, 2))

    def round_four(u):
        for h in range(2):
            first, _, _ = ways(u, h)
            arrive(u, h, *cell(first, 2, 2))

    for step in (1, -1, 2, -2):
        zcopy(z, step).start()
    for k in (1, 2, 3):
        for d in (2 * k - 1, 2 * k):
            zwait(z - d)
            zwait(z + d)
        zcopy(z - 2 * k, 1).start()
        zcopy(z + 2 * k, -1).start()
        zcopy(z - 2 * k, 2).start()
        if k < 3:
            zcopy(z + 2 * k, -2).start()
        if k == 1:
            a2a_home()
        for d in (2 * k - 1, 2 * k):
            a2a(d)
            a2a(-d)
        if k == 2:
            launch(0)
        if k == 3:
            round_one(0)
    zwait(z - 7)
    zwait(z + 7)
    zwait(z - 8)
    a2a(7)
    a2a(-7)
    a2a(8)
    launch(1)
    launch(2)
    round_two(0)
    launch(3)
    round_one(1)
    round_one(2)
    round_three(0)
    round_one(3)
    round_two(1)
    round_two(2)
    round_four(0)
    round_two(3)
    round_three(1)
    round_three(2)
    round_three(3)
    round_four(1)
    round_four(2)
    round_four(3)

    swap.wait_send()
    put.wait()
    pltpu.make_async_copy(xg.at[pl.ds(0, 63)], xg.at[pl.ds(0, 63)], a_send).wait()
    pltpu.make_async_copy(r_out.at[pl.ds(0, 63)], r_out.at[pl.ds(0, 63)], a_recv).wait()
    pltpu.make_async_copy(zbuf.at[pl.ds(0, 15)], zbuf.at[pl.ds(0, 15)], zsend).wait()
    sent = wbuf.at[pl.ds(0, 60 * UNIT)]
    pltpu.make_async_copy(sent, sent, p_send).wait()
    pltpu.make_async_copy(wbuf, wbuf, d_send).wait()
    half = w_out.at[pl.ds(0, 8 * D)]
    pltpu.make_async_copy(half, half, d_recv).wait()
    pltpu.make_async_copy(wbuf, half, h_sem).wait()


def gather_all(ws, xg):
    dma = pltpu.SemaphoreType.DMA
    return pl.pallas_call(
        gather_kernel,
        out_shape=(
            jax.ShapeDtypeStruct((NCH * D, CH), BF16),
            jax.ShapeDtypeStruct((64, 4, D), BF16),
        ),
        in_specs=[pl.BlockSpec(memory_space=pl.ANY)] * 2,
        out_specs=(pl.BlockSpec(memory_space=pl.ANY),) * 2,
        scratch_shapes=[
            pltpu.VMEM((NZ, 2, 54, 128), BF16),
            pltpu.VMEM((8 * D, CH), BF16),
            pltpu.VMEM((4, D), BF16),
            dma((3,)), dma, dma, dma, dma((NZ,)), dma, dma,
            dma, dma((128,)), dma, dma, dma,
        ],
        compiler_params=pltpu.CompilerParams(
            collective_id=0, has_side_effects=True, vmem_limit_bytes=40 << 20
        ),
        name="gather_all",
    )(ws, xg)


NT = (((1,), (1,)), ((), ()))
TN = (((0,), (0,)), ((), ()))
NN = (((1,), (0,)), ((), ()))


def mm(a, b, dims):
    return lax.dot_general(a, b, dims, preferred_element_type=F32)


def softmax_of(qh, kh, factor, mask):
    scores = mm(qh, kh, NT) * factor
    if mask is not None:
        scores = jnp.where(mask, scores, -jnp.inf)
    top = jnp.max(scores, axis=-1, keepdims=True)
    e = jnp.exp(scores - top)
    return e / jnp.sum(e, axis=-1, keepdims=True)


def grads_of(weights, qh, kh, vh, gh, factor):
    grad_value = mm(weights.astype(BF16), gh, TN)
    grad_weight = mm(gh, vh, NT)
    r = jnp.sum(weights * grad_weight, axis=-1, keepdims=True)
    gs = (weights * (grad_weight - r) * factor).astype(BF16)
    grad_query = mm(gs, kh, NN)
    grad_key = mm(gs, qh, TN)
    return grad_query.astype(BF16), grad_key.astype(BF16), grad_value.astype(BF16)


def rest_kernel(
    tokens, r_ref, w_hbm, gain_ref, bias_ref, og_ref, sq_ref, gsum_ref, resid_ref, dqkv_ref, tot_ref,
    wv, qkv_s, g_s, ga_s, dq_s, sw_s, bsrc, brecv, sums, mate, slab, zin, pin, fin,
    wsem, b_send, b_recv, m_send, m_recv, z_send, z_recv, p_send, p_recv, f_send, f_recv,
):
    x, y, z, c = place()
    s, q = lax.axis_index("seq"), lax.axis_index("clip")
    sib = dev(x, y, z, 1 - c)
    barrier = pltpu.get_barrier_semaphore()

    def greet_seq(i, carry):
        pl.semaphore_signal(
            barrier, inc=1, device_id={"clip": q, "seq": (s + i) % 64}, device_id_type=MESH
        )
        return carry

    def xy_peer(i):
        return (x + i // 4) % 4, (y + i % 4) % 4

    def greet_xy(i, carry):
        pl.semaphore_signal(barrier, inc=1, device_id=dev(*xy_peer(i), z, c), device_id_type=MESH)
        return carry

    lax.fori_loop(1, 64, greet_seq, 0)
    lax.fori_loop(1, 16, greet_xy, 0)

    sums[8:16, :] = jnp.zeros((8, D), F32)
    slab[...] = jnp.zeros((NZ, 8, 128), F32)
    head_dim = D // HEADS
    factor = 1.0 / math.sqrt(head_dim)
    copies = []
    for j in range(15):
        cp = pltpu.make_async_copy(w_hbm.at[pl.ds(j * D, D)], wv.at[pl.ds(j * D, D)], wsem.at[j])
        cp.start()
        copies.append(cp)
    rows = r_ref[...].astype(F32)
    xr = rows[:, 0:2, :].reshape(128, D)
    g = rows[:, 2:4, :].reshape(128, D)
    sums[4:5, :] = jnp.sum(g, axis=0, keepdims=True)
    g_s[...] = g.astype(BF16)
    mean = jnp.mean(xr, axis=-1, keepdims=True)
    centred = xr - mean
    inv_std = lax.rsqrt(jnp.mean(centred * centred, axis=-1, keepdims=True) + EPS)
    normal = centred * inv_std
    gain = gain_ref[...]
    normed = (normal * gain).astype(BF16)
    for j in range(9):
        copies[j].wait()
        qkv_s[:, CH * j : CH * j + CH] = (
            mm(normed, wv[j * D : j * D + D, :], NN) + bias_ref[:, CH * j : CH * j + CH]
        ).astype(BF16)
    acc = None
    for j in range(3):
        copies[9 + j].wait()
        part = mm(g_s[:, CH * j : CH * j + CH], wv[(9 + j) * D : (10 + j) * D, :], NT)
        acc = part if acc is None else acc + part
    ga_s[...] = acc.astype(BF16)
    ri = lax.broadcasted_iota(jnp.int32, (128, 128), 0)
    ci = lax.broadcasted_iota(jnp.int32, (128, 128), 1)
    mask = (ri & 1) == (ci & 1)
    for h in range(HEADS):
        lo, hi = h * head_dim, (h + 1) * head_dim
        qh, kh = qkv_s[:, lo:hi], qkv_s[:, D + lo : D + hi]
        gq, gk, gv = grads_of(
            softmax_of(qh, kh, factor, mask), qh, kh, qkv_s[:, 2 * D + lo : 2 * D + hi],
            ga_s[:, lo:hi], factor,
        )
        dq_s[:, lo:hi] = gq
        dq_s[:, D + lo : D + hi] = gk
        dq_s[:, 2 * D + lo : 2 * D + hi] = gv
    acc = None
    for j in range(9):
        part = mm(dq_s[:, CH * j : CH * j + CH], wv[j * D : j * D + D, :], NT)
        acc = part if acc is None else acc + part
    grad_normed = acc
    hat = grad_normed * gain
    branch = inv_std * (
        hat
        - jnp.mean(hat, axis=-1, keepdims=True)
        - normal * jnp.mean(hat * normal, axis=-1, keepdims=True)
    )
    bsrc[...] = branch.reshape(64, 2, D).astype(BF16)

    pl.semaphore_wait(barrier, 78)
    ylo = s // 32
    for dz in (8, 7, 9, 6, 10, 5, 11, 4, 12, 3, 13, 2, 14, 1, 15):
        zz = (z + dz) % NZ

        def back(i, carry):
            t = ((ylo + i // 2) % 2) * 32 + zz * 2 + (c + i) % 2
            pltpu.make_async_remote_copy(
                bsrc.at[t], brecv.at[s], b_send, b_recv,
                device_id={"clip": q, "seq": t}, device_id_type=MESH,
            ).start()
            return carry

        lax.fori_loop(0, 4, back, 0)
    for yl, cc in ((1 - ylo, c), (1 - ylo, 1 - c), (ylo, 1 - c)):
        t = yl * 32 + z * 2 + cc
        pltpu.make_async_remote_copy(
            bsrc.at[t], brecv.at[s], b_send, b_recv,
            device_id={"clip": q, "seq": t}, device_id_type=MESH,
        ).start()
    brecv[s] = bsrc[s]

    sums[0:1, :] = jnp.sum(grad_normed * normal, axis=0, keepdims=True)
    for j in range(3):
        sums[1 + j : 2 + j, :] = jnp.sum(
            dq_s[:, D * j : D * j + D].astype(F32), axis=0, keepdims=True
        )
    for h in range(HEADS):
        lo, hi = h * head_dim, (h + 1) * head_dim
        sw_s[h] = softmax_of(sq_ref[:, lo:hi], sq_ref[:, D + lo : D + hi], factor, None)
    for j in range(12, 15):
        copies[j].wait()

    pltpu.make_async_copy(brecv.at[pl.ds(0, 63)], brecv.at[pl.ds(0, 63)], b_recv).wait()
    resid = (og_ref[...].astype(F32) + brecv[...].astype(F32).reshape(128, D)).astype(BF16)
    resid_ref[...] = resid
    sums[8:9, :] = jnp.sum(resid.astype(F32), axis=0, keepdims=True)
    acc = None
    for j in range(3):
        part = mm(resid_ref[:, CH * j : CH * j + CH], wv[(12 + j) * D : (13 + j) * D, :], NT)
        acc = part if acc is None else acc + part
    ga_s[...] = acc.astype(BF16)
    for h in range(HEADS):
        lo, hi = h * head_dim, (h + 1) * head_dim
        gq, gk, gv = grads_of(
            sw_s[h], sq_ref[:, lo:hi], sq_ref[:, D + lo : D + hi],
            sq_ref[:, 2 * D + lo : 2 * D + hi], ga_s[:, lo:hi], factor,
        )
        dqkv_ref[:, lo:hi] = gq
        dqkv_ref[:, D + lo : D + hi] = gk
        dqkv_ref[:, 2 * D + lo : 2 * D + hi] = gv
    for j in range(3):
        sums[5 + j : 6 + j, :] = jnp.sum(
            dqkv_ref[:, D * j : D * j + D].astype(F32), axis=0, keepdims=True
        )

    swap = pltpu.make_async_remote_copy(
        sums, mate, m_send, m_recv, device_id=sib, device_id_type=MESH
    )
    swap.start()
    swap.wait_recv()
    both = sums[...] + mate[...]
    mine = jnp.where(c == 0, both[0:8], jnp.concatenate([both[5:9], both[9:13]], axis=0))
    for k in range(NZ):
        for yl in range(2):
            lo = yl * 576 + 36 * k
            slab[k, :, 36 * yl : 36 * yl + 36] = mine[:, lo : lo + 36]

    def zsend(i, carry):
        k = (z + i) % NZ
        pltpu.make_async_remote_copy(
            slab.at[k], zin.at[z], z_send, z_recv, device_id=dev(x, y, k, c), device_id_type=MESH
        ).start()
        return carry

    def psend(i, carry):
        pltpu.make_async_remote_copy(
            zin.at[NZ], pin.at[x * 4 + y], p_send, p_recv,
            device_id=dev(*xy_peer(i), z, c), device_id_type=MESH,
        ).start()
        return carry

    lax.fori_loop(1, 16, zsend, 0)
    zin[z] = slab[z]
    pltpu.make_async_copy(zin.at[pl.ds(0, 15)], zin.at[pl.ds(0, 15)], z_recv).wait()
    zsum = jnp.sum(zin[0:NZ], axis=0)
    zin[NZ] = zsum
    lax.fori_loop(1, 16, psend, 0)
    pin[x * 4 + y] = zsum
    pltpu.make_async_copy(pin.at[pl.ds(0, 15)], pin.at[pl.ds(0, 15)], p_recv).wait()
    psum = jnp.sum(pin[...], axis=0)
    fin[c] = psum
    last = pltpu.make_async_remote_copy(
        fin.at[c], fin.at[c], f_send, f_recv, device_id=sib, device_id_type=MESH
    )
    last.start()
    pltpu.make_async_remote_copy(
        fin.at[c], fin.at[1 - c], f_send, f_recv, device_id=sib, device_id_type=MESH
    ).wait_recv()
    total = jnp.concatenate([fin[0, 0:5], fin[1, 0:4]], axis=0)
    part = ylo * 2 + c
    pick = total[:, 0:18]
    for k in range(1, 4):
        pick = jnp.where(part == k, total[:, 18 * k : 18 * k + 18], pick)
    tot_ref[...] = gsum_ref[...] + pick * (1.0 / math.sqrt(tokens))

    swap.wait_send()
    last.wait_send()
    pltpu.make_async_copy(bsrc.at[pl.ds(0, 63)], bsrc.at[pl.ds(0, 63)], b_send).wait()
    pltpu.make_async_copy(slab.at[pl.ds(0, 15)], slab.at[pl.ds(0, 15)], z_send).wait()
    pltpu.make_async_copy(pin.at[pl.ds(0, 15)], pin.at[pl.ds(0, 15)], p_send).wait()


def rest(r, w, gain, bias, og, sq, gsum, tokens):
    vm = pl.BlockSpec(memory_space=pltpu.VMEM)
    dma = pltpu.SemaphoreType.DMA
    return pl.pallas_call(
        functools.partial(rest_kernel, tokens),
        out_shape=(
            jax.ShapeDtypeStruct((128, D), BF16),
            jax.ShapeDtypeStruct((128, 3 * D), BF16),
            jax.ShapeDtypeStruct((9, D // 64), F32),
        ),
        in_specs=[vm, pl.BlockSpec(memory_space=pl.ANY), vm, vm, vm, vm, vm],
        out_specs=(vm, vm, vm),
        scratch_shapes=[
            pltpu.VMEM((15 * D, CH), BF16),
            pltpu.VMEM((128, 3 * D), BF16),
            pltpu.VMEM((128, D), BF16),
            pltpu.VMEM((128, D), BF16),
            pltpu.VMEM((128, 3 * D), BF16),
            pltpu.VMEM((HEADS, 128, 128), F32),
            pltpu.VMEM((64, 2, D), BF16),
            pltpu.VMEM((64, 2, D), BF16),
            pltpu.VMEM((16, D), F32),
            pltpu.VMEM((16, D), F32),
            pltpu.VMEM((NZ, 8, 128), F32),
            pltpu.VMEM((NZ + 1, 8, 128), F32),
            pltpu.VMEM((16, 8, 128), F32),
            pltpu.VMEM((2, 8, 128), F32),
            dma((15,)), dma, dma, dma, dma, dma, dma, dma, dma, dma, dma,
        ],
        compiler_params=pltpu.CompilerParams(
            collective_id=1, has_side_effects=True, vmem_limit_bytes=56 << 20
        ),
        name="rest",
    )(r, w, gain, bias, og, sq, gsum)


def prepare(block_input, out_grad, qkv_weight, out_weight, spatial_out_weight):
    rows = qkv_weight.shape[0]
    pad = jnp.zeros((rows, CH), BF16)
    w = jnp.concatenate([qkv_weight, out_weight, spatial_out_weight, pad], axis=1)
    ws = w.reshape(rows, NCH, 3, 128).transpose(1, 2, 0, 3).reshape(NCH, 3 * rows, 128)
    xg = jnp.concatenate([block_input.reshape(64, 2, D), out_grad.reshape(64, 2, D)], axis=1)
    return ws, xg


def per_device(
    block_input, out_grad, spatial_qkv, norm_gain, qkv_weight, qkv_bias, out_weight,
    spatial_out_weight, grad_sums,
):
    ws, xg = prepare(block_input, out_grad, qkv_weight, out_weight, spatial_out_weight)
    w, r = gather_all(ws, xg)
    tokens = 128 * lax.axis_size("seq") * lax.axis_size("clip")
    resid, sgrad, totals = rest(
        r, w, norm_gain.reshape(1, D), qkv_bias.reshape(1, 3 * D), out_grad.reshape(128, D),
        spatial_qkv.reshape(128, 3 * D), grad_sums, tokens,
    )
    return resid.reshape(1, 1, 128, D), sgrad.reshape(1, 1, 128, 3 * D), totals


def solution(mesh):
    in_specs = (
        P("clip", "seq", None, None),
        P("clip", "seq", None, None),
        P("clip", "seq", None, None),
        P(),
        P("seq", None),
        P(),
        P("seq", None),
        P("seq", None),
        P(None, "seq"),
    )
    out_specs = (P("clip", "seq", None, None), P("clip", "seq", None, None), P(None, "seq"))
    return jax.shard_map(
        per_device, mesh=mesh, in_specs=in_specs, out_specs=out_specs, check_vma=False
    )
```

```python
import functools
import math

import jax
import jax.numpy as jnp
from jax import lax
from jax.experimental import pallas as pl
from jax.experimental.pallas import tpu as pltpu
from jax.sharding import PartitionSpec as P

HEADS = 16
EPS = 1e-06
MESH = pl.DeviceIdType.MESH
F32 = jnp.float32
BF16 = jnp.bfloat16

D = 1152
CH = 384
NCH = 16
NZ = 16
UNIT = 144
HALF = ((0, 80), (80, 64))


def dev(x, y, z, c):
    return {"clip": x * 2 + y // 2, "seq": (y % 2) * 32 + z * 2 + c}


def place():
    s, q = lax.axis_index("seq"), lax.axis_index("clip")
    x = q // 2
    y = (q % 2) * 2 + s // 32
    z = (s // 2) % 16
    c = s % 2
    return x, y, z, c


NT = (((1,), (1,)), ((), ()))
TN = (((0,), (0,)), ((), ()))
NN = (((1,), (0,)), ((), ()))


def mm(a, b, dims):
    return lax.dot_general(a, b, dims, preferred_element_type=F32)


def softmax_of(qh, kh, factor, mask):
    scores = mm(qh, kh, NT) * factor
    if mask is not None:
        scores = jnp.where(mask, scores, -jnp.inf)
    top = jnp.max(scores, axis=-1, keepdims=True)
    e = jnp.exp(scores - top)
    return e / jnp.sum(e, axis=-1, keepdims=True)


def grads_of(weights, qh, kh, vh, gh, factor):
    grad_value = mm(weights.astype(BF16), gh, TN)
    grad_weight = mm(gh, vh, NT)
    r = jnp.sum(weights * grad_weight, axis=-1, keepdims=True)
    gs = (weights * (grad_weight - r) * factor).astype(BF16)
    grad_query = mm(gs, kh, NN)
    grad_key = mm(gs, qh, TN)
    return grad_query.astype(BF16), grad_key.astype(BF16), grad_value.astype(BF16)


WIDE = 640


def sizes(rows):
    return pl.ds(0, rows)


def block_kernel(
    tokens, ws, x_ref, g_ref, sq_ref, gain_ref, bias_ref, gsum_ref, resid_ref, dqkv_ref, tot_ref,
    zbuf, wbuf, asrc, abuf, qkv_s, ga_s, dq_s, sw_s, bsrc, brecv, sums, mate, slab, zin, pin, fin,
    loc, swap_s, swap_r, zg_send, zg_recv, a_send, a_recv, p_send, p_recv, d_send, d_recv,
    b_send, b_recv, m_send, m_recv, z_send, z_recv, q_send, q_recv, f_send, f_recv,
):
    x, y, z, c = place()
    s, q = lax.axis_index("seq"), lax.axis_index("clip")
    ylo = s // 32
    sib = dev(x, y, z, 1 - c)

    def near(axis, step):
        if axis == 0:
            return (x + step + 4) % 4, y
        return x, (y + step + 4) % 4

    def on_line(step):
        return jnp.logical_and(z + step >= 0, z + step < NZ)

    barrier = pltpu.get_barrier_semaphore()
    partners = [
        sib,
        dev(*near(0, 1), z, c),
        dev(*near(0, -1), z, c),
        dev(*near(1, 1), z, c),
        dev(*near(1, -1), z, c),
        {"clip": q, "seq": (1 - ylo) * 32 + z * 2 + 1 - c},
    ]
    for p in partners:
        pl.semaphore_signal(barrier, inc=1, device_id=p, device_id_type=MESH)
    expected = jnp.int32(len(partners))
    for step in (1, -1, 2, -2):
        ok = on_line(step)
        expected = expected + jnp.where(ok, 1, 0)

        @pl.when(ok)
        def _():
            pl.semaphore_signal(
                barrier, inc=1, device_id=dev(x, y, (z + step + NZ) % NZ, c), device_id_type=MESH
            )

    keep = pltpu.make_async_copy(ws.at[2 * q + c], zbuf.at[z, c], loc)
    keep.start()
    sums[...] = jnp.zeros((16, D), F32)
    slab[...] = jnp.zeros((NZ, 8, 128), F32)
    pl.semaphore_wait(barrier, expected)

    swap = pltpu.make_async_remote_copy(
        ws.at[2 * q + 1 - c], zbuf.at[z, c], swap_s, swap_r, device_id=sib, device_id_type=MESH
    )
    swap.start()
    keep.wait()
    pltpu.make_async_remote_copy(
        ws.at[2 * q + 1 - c], zbuf.at[z, 1 - c], swap_s, swap_r, device_id=sib, device_id_type=MESH
    ).wait_recv()

    def zcopy(origin, step):
        o = (origin + 2 * NZ) % NZ
        kind = (0 if abs(step) == 1 else 2) + (0 if step > 0 else 1)
        return pltpu.make_async_remote_copy(
            zbuf.at[o], zbuf.at[o], zg_send.at[kind * NZ + o], zg_recv.at[o],
            device_id=dev(x, y, (z + step + NZ) % NZ, c), device_id_type=MESH,
        )

    def zforward(back, step):
        @pl.when(jnp.logical_and(on_line(back), on_line(step)))
        def _():
            zcopy(z + back, step).start()

    def zwait(back):
        @pl.when(on_line(back))
        def _():
            zcopy(z + back, 1).wait_recv()

    for step in (1, -1, 2, -2):
        zforward(0, step)

    x3 = x_ref[...].astype(F32).reshape(64, 2, D)
    g3 = g_ref[...].astype(F32).reshape(64, 2, D)
    for p in range(2):
        asrc[64 * p : 64 * p + 64] = jnp.concatenate(
            [x3[:, p : p + 1, :], g3[:, p : p + 1, :]], axis=1
        ).astype(BF16)

    def exchange(p, dist):
        @pl.when(on_line(dist))
        def _():
            zz = (z + dist + NZ) % NZ

            def one(i, carry):
                t = ((ylo + i // 2) % 2) * 32 + zz * 2 + (c + i) % 2
                pltpu.make_async_remote_copy(
                    asrc.at[64 * p + t], abuf.at[64 * p + s], a_send, a_recv.at[p],
                    device_id={"clip": q, "seq": t}, device_id_type=MESH,
                ).start()
                return carry

            lax.fori_loop(0, 4, one, 0)

    def exchange_home(p):
        for yl, cc in ((1 - ylo, c), (1 - ylo, 1 - c), (ylo, 1 - c)):
            t = yl * 32 + z * 2 + cc
            pltpu.make_async_remote_copy(
                asrc.at[64 * p + t], abuf.at[64 * p + s], a_send, a_recv.at[p],
                device_id={"clip": q, "seq": t}, device_id_type=MESH,
            ).start()
        abuf[64 * p + s] = asrc[64 * p + s]

    group = z // 4
    order = [group, group + 1 - 2 * (group % 2), 2 - group // 2, 3 - 3 * (group // 2)]

    def spot(u, h, xx, yy):
        off, n = HALF[h]
        at = (2 * (xx * 2 + yy // 2) + c) * D + (yy % 2) * 576 + order[u] * UNIT + off
        return pl.ds(pl.multiple_of(at, 16), n)

    def push(u, h, xx, yy, axis, step):
        rows = spot(u, h, xx, yy)
        nx, ny = near(axis, step)
        pltpu.make_async_remote_copy(
            wbuf.at[rows], wbuf.at[rows], p_send, p_recv.at[(u * 2 + h) * 16 + xx * 4 + yy],
            device_id=dev(nx, ny, z, c), device_id_type=MESH,
        ).start()

    def deliver(u, h, xx, yy):
        rows = spot(u, h, xx, yy)
        pltpu.make_async_remote_copy(
            wbuf.at[rows], wbuf.at[rows], d_send, d_recv, device_id=sib, device_id_type=MESH
        ).start()

    def arrive(u, h, xx, yy):
        rows = spot(u, h, xx, yy)
        pltpu.make_async_remote_copy(
            wbuf.at[rows], wbuf.at[rows], p_send, p_recv.at[(u * 2 + h) * 16 + xx * 4 + yy],
            device_id=sib, device_id_type=MESH,
        ).wait_recv()
        deliver(u, h, xx, yy)

    def cell(axis, a, b):
        if axis == 0:
            return (x + a + 4) % 4, (y + b + 4) % 4
        return (x + b + 4) % 4, (y + a + 4) % 4

    def ways(u, h):
        first = (u + h) % 2
        return first, 1 - first, (1 if (u // 2 + h) % 2 == 0 else -1)

    def launch(u):
        for t in range(3):
            parts = []
            for zi in range(4):
                for cc in range(2):
                    parts.append(zbuf[order[u] * 4 + zi, cc, 18 * t : 18 * t + 18, :].astype(F32))
            at = (2 * q + c) * D + ylo * 576 + order[u] * UNIT
            wbuf[pl.ds(pl.multiple_of(at, 16), UNIT), 128 * t : 128 * t + 128] = jnp.concatenate(
                parts, axis=0
            ).astype(BF16)
        for h in range(2):
            first, second, _ = ways(u, h)
            for step in (1, -1):
                push(u, h, x, y, first, step)
            for step in (1, -1):
                push(u, h, x, y, second, step)
            deliver(u, h, x, y)

    def round_one(u):
        for h in range(2):
            first, second, f = ways(u, h)
            for a in (-f, f):
                blk = cell(first, a, 0)
                arrive(u, h, *blk)
                if a == -f:
                    push(u, h, *blk, first, f)
                for step in (1, -1):
                    push(u, h, *blk, second, step)
            for b in (-f, f):
                blk = cell(first, 0, b)
                arrive(u, h, *blk)
                if b == -f:
                    push(u, h, *blk, second, f)

    def round_two(u):
        for h in range(2):
            first, second, f = ways(u, h)
            blk = cell(first, 2, 0)
            arrive(u, h, *blk)
            for step in (1, -1):
                push(u, h, *blk, second, step)
            for a in (-f, f):
                for b in (-f, f):
                    blk = cell(first, a, b)
                    arrive(u, h, *blk)
                    if b == -f:
                        push(u, h, *blk, second, f)

    def round_three(u):
        for h in range(2):
            first, second, f = ways(u, h)
            arrive(u, h, *cell(first, 0, 2))
            for b in (-f, f):
                blk = cell(first, 2, b)
                arrive(u, h, *blk)
                if b == -f:
                    push(u, h, *blk, second, f)
            for a in (-f, f):
                arrive(u, h, *cell(first, a, 2))

    def round_four(u):
        for h in range(2):
            first, _, _ = ways(u, h)
            arrive(u, h, *cell(first, 2, 2))

    def zstep(k):
        for d in (2 * k - 1, 2 * k):
            zwait(-d)
            zwait(d)
        for step in (1, 2):
            zforward(-2 * k, step)
            zforward(2 * k, -step)
        for d in (2 * k - 1, 2 * k):
            exchange(0, d)
            exchange(0, -d)

    exchange_home(0)
    zstep(1)
    zstep(2)
    launch(0)
    zstep(3)
    round_one(0)
    zstep(4)
    launch(1)
    round_two(0)
    zstep(5)
    round_one(1)
    round_three(0)
    zstep(6)
    launch(2)
    round_two(1)
    zstep(7)
    round_one(2)
    zwait(-15)
    zwait(15)
    exchange(0, 15)
    exchange(0, -15)
    launch(3)
    exchange_home(1)
    for d in range(1, NZ):
        exchange(1, d)
        exchange(1, -d)
    round_four(0)
    round_three(1)
    round_two(2)
    round_one(3)
    round_four(1)
    round_three(2)
    round_two(3)
    round_four(2)
    round_three(3)
    round_four(3)
    half = wbuf.at[sizes(8 * D)]
    pltpu.make_async_copy(half, half, d_recv).wait()

    head_dim = D // HEADS
    factor = 1.0 / math.sqrt(head_dim)
    gain = gain_ref[...]

    def temporal(p):
        arrived = abuf.at[sizes(63)]
        pltpu.make_async_copy(arrived, arrived, a_recv.at[p]).wait()
        rows = abuf[64 * p : 64 * p + 64].astype(F32)
        xr = rows[:, 0:1, :].reshape(64, D)
        g = rows[:, 1:2, :].reshape(64, D)
        gh = g.astype(BF16)
        mean = jnp.mean(xr, axis=-1, keepdims=True)
        centred = xr - mean
        inv_std = lax.rsqrt(jnp.mean(centred * centred, axis=-1, keepdims=True) + EPS)
        normal = centred * inv_std
        normed = (normal * gain).astype(BF16)
        for j in range(9):
            qkv_s[:, CH * j : CH * j + CH] = (
                mm(normed, wbuf[j * D : j * D + D, :], NN) + bias_ref[:, CH * j : CH * j + CH]
            ).astype(BF16)
        acc = None
        for j in range(3):
            part = mm(gh[:, CH * j : CH * j + CH], wbuf[(9 + j) * D : (10 + j) * D, :], NT)
            acc = part if acc is None else acc + part
        ga_s[0:64, :] = acc.astype(BF16)
        for h in range(HEADS):
            lo, hi = h * head_dim, (h + 1) * head_dim
            qh, kh = qkv_s[:, lo:hi], qkv_s[:, D + lo : D + hi]
            gq, gk, gv = grads_of(
                softmax_of(qh, kh, factor, None), qh, kh, qkv_s[:, 2 * D + lo : 2 * D + hi],
                ga_s[0:64, lo:hi], factor,
            )
            dq_s[:, lo:hi] = gq
            dq_s[:, D + lo : D + hi] = gk
            dq_s[:, 2 * D + lo : 2 * D + hi] = gv
        acc = None
        for j in range(9):
            part = mm(dq_s[:, CH * j : CH * j + CH], wbuf[j * D : j * D + D, :], NT)
            acc = part if acc is None else acc + part
        hat = acc * gain
        branch = inv_std * (
            hat
            - jnp.mean(hat, axis=-1, keepdims=True)
            - normal * jnp.mean(hat * normal, axis=-1, keepdims=True)
        )
        low = branch[:, :WIDE].reshape(64, 1, WIDE)
        high = jnp.concatenate(
            [branch[:, WIDE:], jnp.zeros((64, 2 * WIDE - D), F32)], axis=1
        ).reshape(64, 1, WIDE)
        bsrc[64 * p : 64 * p + 64] = jnp.concatenate([low, high], axis=1).astype(BF16)
        for dz in (8, 7, 9, 6, 10, 5, 11, 4, 12, 3, 13, 2, 14, 1, 15):
            zz = (z + dz) % NZ

            def back(i, carry):
                t = ((ylo + i // 2) % 2) * 32 + zz * 2 + (c + i) % 2
                pltpu.make_async_remote_copy(
                    bsrc.at[64 * p + t], brecv.at[64 * p + s], b_send, b_recv,
                    device_id={"clip": q, "seq": t}, device_id_type=MESH,
                ).start()
                return carry

            lax.fori_loop(0, 4, back, 0)
        for yl, cc in ((1 - ylo, c), (1 - ylo, 1 - c), (ylo, 1 - c)):
            t = yl * 32 + z * 2 + cc
            pltpu.make_async_remote_copy(
                bsrc.at[64 * p + t], brecv.at[64 * p + s], b_send, b_recv,
                device_id={"clip": q, "seq": t}, device_id_type=MESH,
            ).start()
        brecv[64 * p + s] = bsrc[64 * p + s]
        sums[0:1, :] += jnp.sum(acc * normal, axis=0, keepdims=True)
        for j in range(3):
            sums[1 + j : 2 + j, :] += jnp.sum(
                dq_s[:, D * j : D * j + D].astype(F32), axis=0, keepdims=True
            )

    temporal(0)
    temporal(1)

    sums[4:5, :] = jnp.sum(g_ref[...].astype(F32), axis=0, keepdims=True)
    for h in range(HEADS):
        lo, hi = h * head_dim, (h + 1) * head_dim
        sw_s[h] = softmax_of(sq_ref[:, lo:hi], sq_ref[:, D + lo : D + hi], factor, None)

    everyone = brecv.at[sizes(126)]
    pltpu.make_async_copy(everyone, everyone, b_recv).wait()
    pieces = []
    for p in range(2):
        rows = brecv[64 * p : 64 * p + 64].astype(F32)
        pieces.append(jnp.concatenate([rows[:, 0:1, :], rows[:, 1:2, : D - WIDE]], axis=2))
    branch = jnp.concatenate(pieces, axis=1).reshape(128, D)
    resid = (g_ref[...].astype(F32) + branch).astype(BF16)
    resid_ref[...] = resid
    sums[8:9, :] = jnp.sum(resid.astype(F32), axis=0, keepdims=True)
    acc = None
    for j in range(3):
        part = mm(resid_ref[:, CH * j : CH * j + CH], wbuf[(12 + j) * D : (13 + j) * D, :], NT)
        acc = part if acc is None else acc + part
    ga_s[...] = acc.astype(BF16)
    for h in range(HEADS):
        lo, hi = h * head_dim, (h + 1) * head_dim
        gq, gk, gv = grads_of(
            sw_s[h], sq_ref[:, lo:hi], sq_ref[:, D + lo : D + hi],
            sq_ref[:, 2 * D + lo : 2 * D + hi], ga_s[:, lo:hi], factor,
        )
        dqkv_ref[:, lo:hi] = gq
        dqkv_ref[:, D + lo : D + hi] = gk
        dqkv_ref[:, 2 * D + lo : 2 * D + hi] = gv
    for j in range(3):
        sums[5 + j : 6 + j, :] = jnp.sum(
            dqkv_ref[:, D * j : D * j + D].astype(F32), axis=0, keepdims=True
        )

    pair = pltpu.make_async_remote_copy(
        sums, mate, m_send, m_recv, device_id=sib, device_id_type=MESH
    )
    pair.start()
    pair.wait_recv()
    both = sums[...] + mate[...]
    mine = jnp.where(c == 0, both[0:8], jnp.concatenate([both[5:9], both[9:13]], axis=0))
    for k in range(NZ):
        for yl in range(2):
            lo = yl * 576 + 36 * k
            slab[k, :, 36 * yl : 36 * yl + 36] = mine[:, lo : lo + 36]

    def xy_peer(i):
        return (x + i // 4) % 4, (y + i % 4) % 4

    def zsend(i, carry):
        k = (z + i) % NZ
        pltpu.make_async_remote_copy(
            slab.at[k], zin.at[z], z_send, z_recv, device_id=dev(x, y, k, c), device_id_type=MESH
        ).start()
        return carry

    def psend(i, carry):
        pltpu.make_async_remote_copy(
            zin.at[NZ], pin.at[x * 4 + y], q_send, q_recv,
            device_id=dev(*xy_peer(i), z, c), device_id_type=MESH,
        ).start()
        return carry

    lax.fori_loop(1, 16, zsend, 0)
    zin[z] = slab[z]
    pltpu.make_async_copy(zin.at[pl.ds(0, 15)], zin.at[pl.ds(0, 15)], z_recv).wait()
    zsum = jnp.sum(zin[0:NZ], axis=0)
    zin[NZ] = zsum
    lax.fori_loop(1, 16, psend, 0)
    pin[x * 4 + y] = zsum
    pltpu.make_async_copy(pin.at[pl.ds(0, 15)], pin.at[pl.ds(0, 15)], q_recv).wait()
    psum = jnp.sum(pin[...], axis=0)
    fin[c] = psum
    last = pltpu.make_async_remote_copy(
        fin.at[c], fin.at[c], f_send, f_recv, device_id=sib, device_id_type=MESH
    )
    last.start()
    pltpu.make_async_remote_copy(
        fin.at[c], fin.at[1 - c], f_send, f_recv, device_id=sib, device_id_type=MESH
    ).wait_recv()
    total = jnp.concatenate([fin[0, 0:5], fin[1, 0:4]], axis=0)
    part = ylo * 2 + c
    pick = total[:, 0:18]
    for k in range(1, 4):
        pick = jnp.where(part == k, total[:, 18 * k : 18 * k + 18], pick)
    tot_ref[...] = gsum_ref[...] + pick * (1.0 / math.sqrt(tokens))

    swap.wait_send()
    pair.wait_send()
    last.wait_send()

    def drain(ref, rows, sem):
        view = ref.at[sizes(rows)]
        pltpu.make_async_copy(view, view, sem).wait()

    drain(asrc, 126, a_send)
    drain(bsrc, 126, b_send)
    drain(zin, 15, z_send)
    drain(pin, 15, q_send)
    drain(wbuf, 60 * UNIT, p_send)
    drain(wbuf, 8 * D, d_send)
    for k in range(8):
        for step in (1, -1, 2, -2):
            back = -2 * k if step > 0 else 2 * k

            @pl.when(jnp.logical_and(on_line(back), on_line(step)))
            def _():
                zcopy(z + back, step).wait_send()


def block(ws, x, g, sq, gain, bias, gsum, tokens):
    vm = pl.BlockSpec(memory_space=pltpu.VMEM)
    dma = pltpu.SemaphoreType.DMA
    return pl.pallas_call(
        functools.partial(block_kernel, tokens),
        out_shape=(
            jax.ShapeDtypeStruct((128, D), BF16),
            jax.ShapeDtypeStruct((128, 3 * D), BF16),
            jax.ShapeDtypeStruct((9, D // 64), F32),
        ),
        in_specs=[pl.BlockSpec(memory_space=pl.ANY)] + [vm] * 6,
        out_specs=(vm, vm, vm),
        scratch_shapes=[
            pltpu.VMEM((NZ, 2, 54, 128), BF16),
            pltpu.VMEM((NCH * D, CH), BF16),
            pltpu.VMEM((128, 2, D), BF16),
            pltpu.VMEM((128, 2, D), BF16),
            pltpu.VMEM((64, 3 * D), BF16),
            pltpu.VMEM((128, D), BF16),
            pltpu.VMEM((64, 3 * D), BF16),
            pltpu.VMEM((HEADS, 128, 128), F32),
            pltpu.VMEM((128, 2, WIDE), BF16),
            pltpu.VMEM((128, 2, WIDE), BF16),
            pltpu.VMEM((16, D), F32),
            pltpu.VMEM((16, D), F32),
            pltpu.VMEM((NZ, 8, 128), F32),
            pltpu.VMEM((NZ + 1, 8, 128), F32),
            pltpu.VMEM((16, 8, 128), F32),
            pltpu.VMEM((2, 8, 128), F32),
            dma, dma, dma, dma((4 * NZ,)), dma((NZ,)), dma, dma((2,)), dma, dma((128,)), dma, dma,
            dma, dma, dma, dma, dma, dma, dma, dma, dma, dma,
        ],
        compiler_params=pltpu.CompilerParams(
            collective_id=0, has_side_effects=True, vmem_limit_bytes=56 << 20
        ),
        name="block",
    )(ws, x, g, sq, gain, bias, gsum)


def per_device(
    block_input, out_grad, spatial_qkv, norm_gain, qkv_weight, qkv_bias, out_weight,
    spatial_out_weight, grad_sums,
):
    rows = qkv_weight.shape[0]
    pad = jnp.zeros((rows, CH), BF16)
    w = jnp.concatenate([qkv_weight, out_weight, spatial_out_weight, pad], axis=1)
    ws = w.reshape(rows, NCH, 3, 128).transpose(1, 2, 0, 3).reshape(NCH, 3 * rows, 128)
    tokens = 128 * lax.axis_size("seq") * lax.axis_size("clip")
    resid, sgrad, totals = block(
        ws, block_input.reshape(128, D), out_grad.reshape(128, D), spatial_qkv.reshape(128, 3 * D),
        norm_gain.reshape(1, D), qkv_bias.reshape(1, 3 * D), grad_sums, tokens,
    )
    return resid.reshape(1, 1, 128, D), sgrad.reshape(1, 1, 128, 3 * D), totals


def solution(mesh):
    in_specs = (
        P("clip", "seq", None, None),
        P("clip", "seq", None, None),
        P("clip", "seq", None, None),
        P(),
        P("seq", None),
        P(),
        P("seq", None),
        P("seq", None),
        P(None, "seq"),
    )
    out_specs = (P("clip", "seq", None, None), P("clip", "seq", None, None), P(None, "seq"))
    return jax.shard_map(
        per_device, mesh=mesh, in_specs=in_specs, out_specs=out_specs, check_vma=False
    )
```

```python
import functools
import math

import jax
import jax.numpy as jnp
from jax import lax
from jax.experimental import pallas as pl
from jax.experimental.pallas import tpu as pltpu
from jax.sharding import PartitionSpec as P

HEADS = 16
EPS = 1e-06
MESH = pl.DeviceIdType.MESH
F32 = jnp.float32
BF16 = jnp.bfloat16

D = 1152
CH = 384
NCH = 16
NZ = 16
UNIT = 144
HALF = ((0, 80), (80, 64))


def dev(x, y, z, c):
    return {"clip": x * 2 + y // 2, "seq": (y % 2) * 32 + z * 2 + c}


def place():
    s, q = lax.axis_index("seq"), lax.axis_index("clip")
    x = q // 2
    y = (q % 2) * 2 + s // 32
    z = (s // 2) % 16
    c = s % 2
    return x, y, z, c


NT = (((1,), (1,)), ((), ()))
TN = (((0,), (0,)), ((), ()))
NN = (((1,), (0,)), ((), ()))


def mm(a, b, dims):
    return lax.dot_general(a, b, dims, preferred_element_type=F32)


def softmax_of(qh, kh, factor, mask):
    scores = mm(qh, kh, NT) * factor
    if mask is not None:
        scores = jnp.where(mask, scores, -jnp.inf)
    top = jnp.max(scores, axis=-1, keepdims=True)
    e = jnp.exp(scores - top)
    return e / jnp.sum(e, axis=-1, keepdims=True)


def grads_of(weights, qh, kh, vh, gh, factor):
    grad_value = mm(weights.astype(BF16), gh, TN)
    grad_weight = mm(gh, vh, NT)
    r = jnp.sum(weights * grad_weight, axis=-1, keepdims=True)
    gs = (weights * (grad_weight - r) * factor).astype(BF16)
    grad_query = mm(gs, kh, NN)
    grad_key = mm(gs, qh, TN)
    return grad_query.astype(BF16), grad_key.astype(BF16), grad_value.astype(BF16)


def sizes(rows):
    return pl.ds(0, rows)


def block_kernel(
    tokens, ws, x_ref, g_ref, sq_ref, gain_ref, bias_ref, gsum_ref, resid_ref, dqkv_ref, tot_ref,
    zbuf, wbuf, asrc, abuf, qkv_s, g_s, ga_s, dq_s, sw_s, bsrc, brecv, sums, mate, slab, zin, pin, fin,
    loc, swap_s, swap_r, zg_send, zg_recv, a_send, a_recv, p_send, p_recv, d_send, d_recv,
    b_send, b_recv, m_send, m_recv, z_send, z_recv, q_send, q_recv, f_send, f_recv,
):
    x, y, z, c = place()
    s, q = lax.axis_index("seq"), lax.axis_index("clip")
    ylo = s // 32
    sib = dev(x, y, z, 1 - c)

    def near(axis, step):
        if axis == 0:
            return (x + step + 4) % 4, y
        return x, (y + step + 4) % 4

    barrier = pltpu.get_barrier_semaphore()
    partners = [
        sib,
        dev(*near(0, 1), z, c),
        dev(*near(0, -1), z, c),
        dev(*near(1, 1), z, c),
        dev(*near(1, -1), z, c),
        {"clip": q, "seq": (1 - ylo) * 32 + z * 2 + 1 - c},
        dev(x, y, (z + 1) % NZ, c),
        dev(x, y, (z + NZ - 1) % NZ, c),
        dev(x, y, (z + 2) % NZ, c),
        dev(x, y, (z + NZ - 2) % NZ, c),
    ]
    for p in partners:
        pl.semaphore_signal(barrier, inc=1, device_id=p, device_id_type=MESH)
    keep = pltpu.make_async_copy(ws.at[2 * q + c], zbuf.at[z, c], loc)
    keep.start()
    sums[...] = jnp.zeros((16, D), F32)
    slab[...] = jnp.zeros((NZ, 8, 128), F32)
    pl.semaphore_wait(barrier, len(partners))

    swap = pltpu.make_async_remote_copy(
        ws.at[2 * q + 1 - c], zbuf.at[z, c], swap_s, swap_r, device_id=sib, device_id_type=MESH
    )
    swap.start()
    keep.wait()
    pltpu.make_async_remote_copy(
        ws.at[2 * q + 1 - c], zbuf.at[z, 1 - c], swap_s, swap_r, device_id=sib, device_id_type=MESH
    ).wait_recv()

    def zcopy(origin, step):
        o = (origin + 2 * NZ) % NZ
        return pltpu.make_async_remote_copy(
            zbuf.at[o], zbuf.at[o], zg_send, zg_recv.at[o],
            device_id=dev(x, y, (z + step + NZ) % NZ, c), device_id_type=MESH,
        )

    def zwait(origin):
        zcopy(origin, 1).wait_recv()

    for step in (1, -1, 2, -2):
        zcopy(z, step).start()

    x3 = x_ref[...].astype(F32).reshape(64, 2, D)
    g3 = g_ref[...].astype(F32).reshape(64, 2, D)
    asrc[...] = jnp.concatenate([x3, g3], axis=1).astype(BF16)

    def exchange(dist):
        zz = (z + dist + NZ) % NZ

        def one(i, carry):
            t = ((ylo + i // 2) % 2) * 32 + zz * 2 + (c + i) % 2
            pltpu.make_async_remote_copy(
                asrc.at[t], abuf.at[s], a_send, a_recv,
                device_id={"clip": q, "seq": t}, device_id_type=MESH,
            ).start()
            return carry

        lax.fori_loop(0, 4, one, 0)

    def exchange_home():
        for yl, cc in ((1 - ylo, c), (1 - ylo, 1 - c), (ylo, 1 - c)):
            t = yl * 32 + z * 2 + cc
            pltpu.make_async_remote_copy(
                asrc.at[t], abuf.at[s], a_send, a_recv,
                device_id={"clip": q, "seq": t}, device_id_type=MESH,
            ).start()
        abuf[s] = asrc[s]

    group = z // 4
    order = [group, group + 1 - 2 * (group % 2), 2 - group // 2, 3 - 3 * (group // 2)]

    def spot(u, h, xx, yy):
        off, n = HALF[h]
        at = (2 * (xx * 2 + yy // 2) + c) * D + (yy % 2) * 576 + order[u] * UNIT + off
        return pl.ds(pl.multiple_of(at, 16), n)

    def push(u, h, xx, yy, axis, step):
        rows = spot(u, h, xx, yy)
        nx, ny = near(axis, step)
        pltpu.make_async_remote_copy(
            wbuf.at[rows], wbuf.at[rows], p_send, p_recv.at[(u * 2 + h) * 16 + xx * 4 + yy],
            device_id=dev(nx, ny, z, c), device_id_type=MESH,
        ).start()

    def deliver(u, h, xx, yy):
        rows = spot(u, h, xx, yy)
        pltpu.make_async_remote_copy(
            wbuf.at[rows], wbuf.at[rows], d_send, d_recv, device_id=sib, device_id_type=MESH
        ).start()

    def arrive(u, h, xx, yy):
        rows = spot(u, h, xx, yy)
        pltpu.make_async_remote_copy(
            wbuf.at[rows], wbuf.at[rows], p_send, p_recv.at[(u * 2 + h) * 16 + xx * 4 + yy],
            device_id=sib, device_id_type=MESH,
        ).wait_recv()
        deliver(u, h, xx, yy)

    def cell(axis, a, b):
        if axis == 0:
            return (x + a + 4) % 4, (y + b + 4) % 4
        return (x + b + 4) % 4, (y + a + 4) % 4

    def ways(u, h):
        first = (u + h) % 2
        return first, 1 - first, (1 if (u // 2 + h) % 2 == 0 else -1)

    def launch(u):
        for t in range(3):
            parts = []
            for zi in range(4):
                for cc in range(2):
                    parts.append(zbuf[order[u] * 4 + zi, cc, 18 * t : 18 * t + 18, :].astype(F32))
            at = (2 * q + c) * D + ylo * 576 + order[u] * UNIT
            wbuf[pl.ds(pl.multiple_of(at, 16), UNIT), 128 * t : 128 * t + 128] = jnp.concatenate(
                parts, axis=0
            ).astype(BF16)
        for h in range(2):
            first, second, _ = ways(u, h)
            for step in (1, -1):
                push(u, h, x, y, first, step)
            for step in (1, -1):
                push(u, h, x, y, second, step)
            deliver(u, h, x, y)

    def round_one(u):
        for h in range(2):
            first, second, f = ways(u, h)
            for a in (-f, f):
                blk = cell(first, a, 0)
                arrive(u, h, *blk)
                if a == -f:
                    push(u, h, *blk, first, f)
                for step in (1, -1):
                    push(u, h, *blk, second, step)
            for b in (-f, f):
                blk = cell(first, 0, b)
                arrive(u, h, *blk)
                if b == -f:
                    push(u, h, *blk, second, f)

    def round_two(u):
        for h in range(2):
            first, second, f = ways(u, h)
            blk = cell(first, 2, 0)
            arrive(u, h, *blk)
            for step in (1, -1):
                push(u, h, *blk, second, step)
            for a in (-f, f):
                for b in (-f, f):
                    blk = cell(first, a, b)
                    arrive(u, h, *blk)
                    if b == -f:
                        push(u, h, *blk, second, f)

    def round_three(u):
        for h in range(2):
            first, second, f = ways(u, h)
            arrive(u, h, *cell(first, 0, 2))
            for b in (-f, f):
                blk = cell(first, 2, b)
                arrive(u, h, *blk)
                if b == -f:
                    push(u, h, *blk, second, f)
            for a in (-f, f):
                arrive(u, h, *cell(first, a, 2))

    def round_four(u):
        for h in range(2):
            first, _, _ = ways(u, h)
            arrive(u, h, *cell(first, 2, 2))

    for k in (1, 2, 3):
        for d in (2 * k - 1, 2 * k):
            zwait(z - d)
            zwait(z + d)
        zcopy(z - 2 * k, 1).start()
        zcopy(z + 2 * k, -1).start()
        zcopy(z - 2 * k, 2).start()
        if k < 3:
            zcopy(z + 2 * k, -2).start()
        if k == 1:
            exchange_home()
        for d in (2 * k - 1, 2 * k):
            exchange(d)
            exchange(-d)
        if k == 2:
            launch(0)
        if k == 3:
            round_one(0)
    zwait(z - 7)
    zwait(z + 7)
    zwait(z - 8)
    exchange(7)
    exchange(-7)
    exchange(8)
    launch(1)
    launch(2)
    round_two(0)
    launch(3)
    round_one(1)
    round_one(2)
    round_three(0)
    round_one(3)
    round_two(1)
    round_two(2)
    round_four(0)
    round_two(3)
    round_three(1)
    round_three(2)
    round_three(3)
    round_four(1)
    round_four(2)
    round_four(3)

    head_dim = D // HEADS
    factor = 1.0 / math.sqrt(head_dim)
    arrived = abuf.at[sizes(63)]
    pltpu.make_async_copy(arrived, arrived, a_recv).wait()
    rows = abuf[...].astype(F32)
    xr = rows[:, 0:2, :].reshape(128, D)
    g = rows[:, 2:4, :].reshape(128, D)
    sums[4:5, :] = jnp.sum(g, axis=0, keepdims=True)
    g_s[...] = g.astype(BF16)
    mean = jnp.mean(xr, axis=-1, keepdims=True)
    centred = xr - mean
    inv_std = lax.rsqrt(jnp.mean(centred * centred, axis=-1, keepdims=True) + EPS)
    normal = centred * inv_std
    gain = gain_ref[...].reshape(1, D)
    normed = (normal * gain).astype(BF16)
    half = wbuf.at[sizes(8 * D)]
    pltpu.make_async_copy(half, half, d_recv).wait()
    for j in range(9):
        qkv_s[:, CH * j : CH * j + CH] = (
            mm(normed, wbuf[j * D : j * D + D, :], NN) + bias_ref[CH * j : CH * j + CH].reshape(1, CH)
        ).astype(BF16)
    acc = None
    for j in range(3):
        part = mm(g_s[:, CH * j : CH * j + CH], wbuf[(9 + j) * D : (10 + j) * D, :], NT)
        acc = part if acc is None else acc + part
    ga_s[...] = acc.astype(BF16)
    ri = lax.broadcasted_iota(jnp.int32, (128, 128), 0)
    ci = lax.broadcasted_iota(jnp.int32, (128, 128), 1)
    mask = (ri & 1) == (ci & 1)
    for h in range(HEADS):
        lo, hi = h * head_dim, (h + 1) * head_dim
        qh, kh = qkv_s[:, lo:hi], qkv_s[:, D + lo : D + hi]
        gq, gk, gv = grads_of(
            softmax_of(qh, kh, factor, mask), qh, kh, qkv_s[:, 2 * D + lo : 2 * D + hi],
            ga_s[:, lo:hi], factor,
        )
        dq_s[:, lo:hi] = gq
        dq_s[:, D + lo : D + hi] = gk
        dq_s[:, 2 * D + lo : 2 * D + hi] = gv
    acc = None
    for j in range(9):
        part = mm(dq_s[:, CH * j : CH * j + CH], wbuf[j * D : j * D + D, :], NT)
        acc = part if acc is None else acc + part
    grad_normed = acc
    hat = grad_normed * gain
    branch = inv_std * (
        hat
        - jnp.mean(hat, axis=-1, keepdims=True)
        - normal * jnp.mean(hat * normal, axis=-1, keepdims=True)
    )
    bsrc[...] = branch.reshape(64, 2, D).astype(BF16)

    for dz in (8, 7, 9, 6, 10, 5, 11, 4, 12, 3, 13, 2, 14, 1, 15):
        zz = (z + dz) % NZ

        def back(i, carry):
            t = ((ylo + i // 2) % 2) * 32 + zz * 2 + (c + i) % 2
            pltpu.make_async_remote_copy(
                bsrc.at[t], brecv.at[s], b_send, b_recv,
                device_id={"clip": q, "seq": t}, device_id_type=MESH,
            ).start()
            return carry

        lax.fori_loop(0, 4, back, 0)
    for yl, cc in ((1 - ylo, c), (1 - ylo, 1 - c), (ylo, 1 - c)):
        t = yl * 32 + z * 2 + cc
        pltpu.make_async_remote_copy(
            bsrc.at[t], brecv.at[s], b_send, b_recv,
            device_id={"clip": q, "seq": t}, device_id_type=MESH,
        ).start()
    brecv[s] = bsrc[s]

    sums[0:1, :] = jnp.sum(grad_normed * normal, axis=0, keepdims=True)
    for j in range(3):
        sums[1 + j : 2 + j, :] = jnp.sum(
            dq_s[:, D * j : D * j + D].astype(F32), axis=0, keepdims=True
        )
    for h in range(HEADS):
        lo, hi = h * head_dim, (h + 1) * head_dim
        sw_s[h] = softmax_of(sq_ref[:, lo:hi], sq_ref[:, D + lo : D + hi], factor, None)

    pltpu.make_async_copy(brecv.at[pl.ds(0, 63)], brecv.at[pl.ds(0, 63)], b_recv).wait()
    resid = (g_ref[...].astype(F32) + brecv[...].astype(F32).reshape(128, D)).astype(BF16)
    resid_ref[...] = resid
    sums[8:9, :] = jnp.sum(resid.astype(F32), axis=0, keepdims=True)
    acc = None
    for j in range(3):
        part = mm(resid_ref[:, CH * j : CH * j + CH], wbuf[(12 + j) * D : (13 + j) * D, :], NT)
        acc = part if acc is None else acc + part
    ga_s[...] = acc.astype(BF16)
    for h in range(HEADS):
        lo, hi = h * head_dim, (h + 1) * head_dim
        gq, gk, gv = grads_of(
            sw_s[h], sq_ref[:, lo:hi], sq_ref[:, D + lo : D + hi],
            sq_ref[:, 2 * D + lo : 2 * D + hi], ga_s[:, lo:hi], factor,
        )
        dqkv_ref[:, lo:hi] = gq
        dqkv_ref[:, D + lo : D + hi] = gk
        dqkv_ref[:, 2 * D + lo : 2 * D + hi] = gv
    for j in range(3):
        sums[5 + j : 6 + j, :] = jnp.sum(
            dqkv_ref[:, D * j : D * j + D].astype(F32), axis=0, keepdims=True
        )

    pair = pltpu.make_async_remote_copy(
        sums, mate, m_send, m_recv, device_id=sib, device_id_type=MESH
    )
    pair.start()
    pair.wait_recv()
    both = sums[...] + mate[...]
    mine = jnp.where(c == 0, both[0:8], jnp.concatenate([both[5:9], both[9:13]], axis=0))
    for k in range(NZ):
        for yl in range(2):
            lo = yl * 576 + 36 * k
            slab[k, :, 36 * yl : 36 * yl + 36] = mine[:, lo : lo + 36]

    def xy_peer(i):
        return (x + i // 4) % 4, (y + i % 4) % 4

    def zsend(i, carry):
        k = (z + i) % NZ
        pltpu.make_async_remote_copy(
            slab.at[k], zin.at[z], z_send, z_recv, device_id=dev(x, y, k, c), device_id_type=MESH
        ).start()
        return carry

    def psend(i, carry):
        pltpu.make_async_remote_copy(
            zin.at[NZ], pin.at[x * 4 + y], q_send, q_recv,
            device_id=dev(*xy_peer(i), z, c), device_id_type=MESH,
        ).start()
        return carry

    lax.fori_loop(1, 16, zsend, 0)
    zin[z] = slab[z]
    pltpu.make_async_copy(zin.at[pl.ds(0, 15)], zin.at[pl.ds(0, 15)], z_recv).wait()
    zsum = jnp.sum(zin[0:NZ], axis=0)
    zin[NZ] = zsum
    lax.fori_loop(1, 16, psend, 0)
    pin[x * 4 + y] = zsum
    pltpu.make_async_copy(pin.at[pl.ds(0, 15)], pin.at[pl.ds(0, 15)], q_recv).wait()
    psum = jnp.sum(pin[...], axis=0)
    fin[c] = psum
    last = pltpu.make_async_remote_copy(
        fin.at[c], fin.at[c], f_send, f_recv, device_id=sib, device_id_type=MESH
    )
    last.start()
    pltpu.make_async_remote_copy(
        fin.at[c], fin.at[1 - c], f_send, f_recv, device_id=sib, device_id_type=MESH
    ).wait_recv()
    total = jnp.concatenate([fin[0, 0:5], fin[1, 0:4]], axis=0)
    part = ylo * 2 + c
    pick = total[:, 0:18]
    for k in range(1, 4):
        pick = jnp.where(part == k, total[:, 18 * k : 18 * k + 18], pick)
    tot_ref[...] = gsum_ref[...] + pick * (1.0 / math.sqrt(tokens))

    swap.wait_send()
    pair.wait_send()
    last.wait_send()

    def drain(ref, rows, sem):
        view = ref.at[sizes(rows)]
        pltpu.make_async_copy(view, view, sem).wait()

    drain(asrc, 63, a_send)
    drain(bsrc, 63, b_send)
    drain(zin, 15, z_send)
    drain(pin, 15, q_send)
    drain(wbuf, 60 * UNIT, p_send)
    drain(wbuf, 8 * D, d_send)
    drain(zbuf, 15, zg_send)


def block(ws, x, g, sq, gain, bias, gsum, tokens):
    vm = pl.BlockSpec(memory_space=pltpu.VMEM)
    dma = pltpu.SemaphoreType.DMA
    return pl.pallas_call(
        functools.partial(block_kernel, tokens),
        out_shape=(
            jax.ShapeDtypeStruct((128, D), BF16),
            jax.ShapeDtypeStruct((128, 3 * D), BF16),
            jax.ShapeDtypeStruct((9, D // 64), F32),
        ),
        in_specs=[pl.BlockSpec(memory_space=pl.ANY)] + [vm] * 6,
        out_specs=(vm, vm, vm),
        scratch_shapes=[
            pltpu.VMEM((NZ, 2, 54, 128), BF16),
            pltpu.VMEM((NCH * D, CH), BF16),
            pltpu.VMEM((64, 4, D), BF16),
            pltpu.VMEM((64, 4, D), BF16),
            pltpu.VMEM((128, 3 * D), BF16),
            pltpu.VMEM((128, D), BF16),
            pltpu.VMEM((128, D), BF16),
            pltpu.VMEM((128, 3 * D), BF16),
            pltpu.VMEM((HEADS, 128, 128), F32),
            pltpu.VMEM((64, 2, D), BF16),
            pltpu.VMEM((64, 2, D), BF16),
            pltpu.VMEM((16, D), F32),
            pltpu.VMEM((16, D), F32),
            pltpu.VMEM((NZ, 8, 128), F32),
            pltpu.VMEM((NZ + 1, 8, 128), F32),
            pltpu.VMEM((16, 8, 128), F32),
            pltpu.VMEM((2, 8, 128), F32),
            dma, dma, dma, dma, dma((NZ,)), dma, dma, dma, dma((128,)), dma, dma,
            dma, dma, dma, dma, dma, dma, dma, dma, dma, dma,
        ],
        compiler_params=pltpu.CompilerParams(
            collective_id=0, has_side_effects=True, vmem_limit_bytes=56 << 20
        ),
        name="block",
    )(ws, x, g, sq, gain, bias, gsum)


def per_device(
    block_input, out_grad, spatial_qkv, norm_gain, qkv_weight, qkv_bias, out_weight,
    spatial_out_weight, grad_sums,
):
    rows = qkv_weight.shape[0]
    pad = jnp.zeros((rows, CH), BF16)
    w = jnp.concatenate([qkv_weight, out_weight, spatial_out_weight, pad], axis=1)
    ws = w.reshape(rows, NCH, 3, 128).transpose(1, 2, 0, 3).reshape(NCH, 3 * rows, 128)
    tokens = 128 * lax.axis_size("seq") * lax.axis_size("clip")
    resid, sgrad, totals = block(
        ws, block_input.reshape(128, D), out_grad.reshape(128, D), spatial_qkv.reshape(128, 3 * D),
        norm_gain, qkv_bias, grad_sums, tokens,
    )
    return resid.reshape(1, 1, 128, D), sgrad.reshape(1, 1, 128, 3 * D), totals


def solution(mesh):
    in_specs = (
        P("clip", "seq", None, None),
        P("clip", "seq", None, None),
        P("clip", "seq", None, None),
        P(),
        P("seq", None),
        P(),
        P("seq", None),
        P("seq", None),
        P(None, "seq"),
    )
    out_specs = (P("clip", "seq", None, None), P("clip", "seq", None, None), P(None, "seq"))
    return jax.shard_map(
        per_device, mesh=mesh, in_specs=in_specs, out_specs=out_specs, check_vma=False
    )
```

```python
import functools
import math

import jax
import jax.numpy as jnp
from jax import lax
from jax.experimental import pallas as pl
from jax.experimental.pallas import tpu as pltpu
from jax.sharding import PartitionSpec as P

HEADS = 16
EPS = 1e-06
MESH = pl.DeviceIdType.MESH
F32 = jnp.float32
BF16 = jnp.bfloat16

D = 1152
CH = 384
NCH = 16
NZ = 16
UNIT = 144
HALF = ((0, 80), (80, 64))


def dev(x, y, z, c):
    return {"clip": x * 2 + y // 2, "seq": (y % 2) * 32 + z * 2 + c}


def place():
    s, q = lax.axis_index("seq"), lax.axis_index("clip")
    x = q // 2
    y = (q % 2) * 2 + s // 32
    z = (s // 2) % 16
    c = s % 2
    return x, y, z, c


NT = (((1,), (1,)), ((), ()))
TN = (((0,), (0,)), ((), ()))
NN = (((1,), (0,)), ((), ()))


def mm(a, b, dims):
    return lax.dot_general(a, b, dims, preferred_element_type=F32)


def softmax_of(qh, kh, factor, mask):
    scores = mm(qh, kh, NT) * factor
    if mask is not None:
        scores = jnp.where(mask, scores, -jnp.inf)
    top = jnp.max(scores, axis=-1, keepdims=True)
    e = jnp.exp(scores - top)
    return e / jnp.sum(e, axis=-1, keepdims=True)


def grads_of(weights, qh, kh, vh, gh, factor):
    grad_value = mm(weights.astype(BF16), gh, TN)
    grad_weight = mm(gh, vh, NT)
    r = jnp.sum(weights * grad_weight, axis=-1, keepdims=True)
    gs = (weights * (grad_weight - r) * factor).astype(BF16)
    grad_query = mm(gs, kh, NN)
    grad_key = mm(gs, qh, TN)
    return grad_query.astype(BF16), grad_key.astype(BF16), grad_value.astype(BF16)


def sizes(rows):
    return pl.ds(0, rows)


def block_kernel(
    tokens, ws, x_ref, g_ref, sq_ref, gain_ref, bias_ref, resid_ref, dqkv_ref, tot_ref,
    zbuf, wbuf, asrc, abuf, qkv_s, g_s, ga_s, dq_s, sw_s, bsrc, brecv, sums, mate, slab, zin, pin, fin,
    loc, swap_s, swap_r, zg_send, zg_recv, a_send, a_recv, p_send, p_recv, d_send, d_recv,
    b_send, b_recv, m_send, m_recv, z_send, z_recv, q_send, q_recv, f_send, f_recv,
):
    x, y, z, c = place()
    s, q = lax.axis_index("seq"), lax.axis_index("clip")
    ylo = s // 32
    sib = dev(x, y, z, 1 - c)

    def near(axis, step):
        if axis == 0:
            return (x + step + 4) % 4, y
        return x, (y + step + 4) % 4

    barrier = pltpu.get_barrier_semaphore()
    partners = [
        sib,
        dev(*near(0, 1), z, c),
        dev(*near(0, -1), z, c),
        dev(*near(1, 1), z, c),
        dev(*near(1, -1), z, c),
        {"clip": q, "seq": (1 - ylo) * 32 + z * 2 + 1 - c},
        dev(x, y, (z + 1) % NZ, c),
        dev(x, y, (z + NZ - 1) % NZ, c),
        dev(x, y, (z + 2) % NZ, c),
        dev(x, y, (z + NZ - 2) % NZ, c),
    ]
    for p in partners:
        pl.semaphore_signal(barrier, inc=1, device_id=p, device_id_type=MESH)
    keep = pltpu.make_async_copy(ws.at[2 * q + c], zbuf.at[z, c], loc)
    keep.start()
    sums[...] = jnp.zeros((16, D), F32)
    slab[...] = jnp.zeros((NZ, 8, 128), F32)
    pl.semaphore_wait(barrier, len(partners))

    swap = pltpu.make_async_remote_copy(
        ws.at[2 * q + 1 - c], zbuf.at[z, c], swap_s, swap_r, device_id=sib, device_id_type=MESH
    )
    swap.start()
    keep.wait()
    pltpu.make_async_remote_copy(
        ws.at[2 * q + 1 - c], zbuf.at[z, 1 - c], swap_s, swap_r, device_id=sib, device_id_type=MESH
    ).wait_recv()

    def zcopy(origin, step):
        o = (origin + 2 * NZ) % NZ
        return pltpu.make_async_remote_copy(
            zbuf.at[o], zbuf.at[o], zg_send, zg_recv.at[o],
            device_id=dev(x, y, (z + step + NZ) % NZ, c), device_id_type=MESH,
        )

    def zwait(origin):
        zcopy(origin, 1).wait_recv()

    for step in (1, -1, 2, -2):
        zcopy(z, step).start()

    x3 = x_ref[...].astype(F32).reshape(64, 2, D)
    g3 = g_ref[...].astype(F32).reshape(64, 2, D)
    asrc[...] = jnp.concatenate([x3, g3], axis=1).astype(BF16)

    def exchange(dist):
        zz = (z + dist + NZ) % NZ

        def one(i, carry):
            t = ((ylo + i // 2) % 2) * 32 + zz * 2 + (c + i) % 2
            pltpu.make_async_remote_copy(
                asrc.at[t], abuf.at[s], a_send, a_recv,
                device_id={"clip": q, "seq": t}, device_id_type=MESH,
            ).start()
            return carry

        lax.fori_loop(0, 4, one, 0)

    def exchange_home():
        for yl, cc in ((1 - ylo, c), (1 - ylo, 1 - c), (ylo, 1 - c)):
            t = yl * 32 + z * 2 + cc
            pltpu.make_async_remote_copy(
                asrc.at[t], abuf.at[s], a_send, a_recv,
                device_id={"clip": q, "seq": t}, device_id_type=MESH,
            ).start()
        abuf[s] = asrc[s]

    group = z // 4
    order = [group, group + 1 - 2 * (group % 2), 2 - group // 2, 3 - 3 * (group // 2)]

    def spot(u, h, xx, yy):
        off, n = HALF[h]
        at = (2 * (xx * 2 + yy // 2) + c) * D + (yy % 2) * 576 + order[u] * UNIT + off
        return pl.ds(pl.multiple_of(at, 16), n)

    def push(u, h, xx, yy, axis, step):
        rows = spot(u, h, xx, yy)
        nx, ny = near(axis, step)
        pltpu.make_async_remote_copy(
            wbuf.at[rows], wbuf.at[rows], p_send, p_recv.at[(u * 2 + h) * 16 + xx * 4 + yy],
            device_id=dev(nx, ny, z, c), device_id_type=MESH,
        ).start()

    def deliver(u, h, xx, yy):
        rows = spot(u, h, xx, yy)
        pltpu.make_async_remote_copy(
            wbuf.at[rows], wbuf.at[rows], d_send, d_recv, device_id=sib, device_id_type=MESH
        ).start()

    def arrive(u, h, xx, yy):
        rows = spot(u, h, xx, yy)
        pltpu.make_async_remote_copy(
            wbuf.at[rows], wbuf.at[rows], p_send, p_recv.at[(u * 2 + h) * 16 + xx * 4 + yy],
            device_id=sib, device_id_type=MESH,
        ).wait_recv()
        deliver(u, h, xx, yy)

    def cell(axis, a, b):
        if axis == 0:
            return (x + a + 4) % 4, (y + b + 4) % 4
        return (x + b + 4) % 4, (y + a + 4) % 4

    def ways(u, h):
        first = (u + h) % 2
        return first, 1 - first, (1 if (u // 2 + h) % 2 == 0 else -1)

    def launch(u):
        for t in range(3):
            parts = []
            for zi in range(4):
                for cc in range(2):
                    parts.append(zbuf[order[u] * 4 + zi, cc, 18 * t : 18 * t + 18, :].astype(F32))
            at = (2 * q + c) * D + ylo * 576 + order[u] * UNIT
            wbuf[pl.ds(pl.multiple_of(at, 16), UNIT), 128 * t : 128 * t + 128] = jnp.concatenate(
                parts, axis=0
            ).astype(BF16)
        for h in range(2):
            first, second, _ = ways(u, h)
            for step in (1, -1):
                push(u, h, x, y, first, step)
            for step in (1, -1):
                push(u, h, x, y, second, step)
            deliver(u, h, x, y)

    def round_one(u):
        for h in range(2):
            first, second, f = ways(u, h)
            for a in (-f, f):
                blk = cell(first, a, 0)
                arrive(u, h, *blk)
                if a == -f:
                    push(u, h, *blk, first, f)
                for step in (1, -1):
                    push(u, h, *blk, second, step)
            for b in (-f, f):
                blk = cell(first, 0, b)
                arrive(u, h, *blk)
                if b == -f:
                    push(u, h, *blk, second, f)

    def round_two(u):
        for h in range(2):
            first, second, f = ways(u, h)
            blk = cell(first, 2, 0)
            arrive(u, h, *blk)
            for step in (1, -1):
                push(u, h, *blk, second, step)
            for a in (-f, f):
                for b in (-f, f):
                    blk = cell(first, a, b)
                    arrive(u, h, *blk)
                    if b == -f:
                        push(u, h, *blk, second, f)

    def round_three(u):
        for h in range(2):
            first, second, f = ways(u, h)
            arrive(u, h, *cell(first, 0, 2))
            for b in (-f, f):
                blk = cell(first, 2, b)
                arrive(u, h, *blk)
                if b == -f:
                    push(u, h, *blk, second, f)
            for a in (-f, f):
                arrive(u, h, *cell(first, a, 2))

    def round_four(u):
        for h in range(2):
            first, _, _ = ways(u, h)
            arrive(u, h, *cell(first, 2, 2))

    for k in (1, 2, 3):
        for d in (2 * k - 1, 2 * k):
            zwait(z - d)
            zwait(z + d)
        zcopy(z - 2 * k, 1).start()
        zcopy(z + 2 * k, -1).start()
        zcopy(z - 2 * k, 2).start()
        if k < 3:
            zcopy(z + 2 * k, -2).start()
        if k == 1:
            exchange_home()
        for d in (2 * k - 1, 2 * k):
            exchange(d)
            exchange(-d)
        if k == 2:
            launch(0)
        if k == 3:
            round_one(0)
    zwait(z - 7)
    zwait(z + 7)
    zwait(z - 8)
    exchange(7)
    exchange(-7)
    exchange(8)
    launch(1)
    launch(2)
    round_two(0)
    launch(3)
    round_one(1)
    round_one(2)
    round_three(0)
    round_one(3)
    round_two(1)
    round_two(2)
    round_four(0)
    round_two(3)
    round_three(1)
    round_three(2)
    round_three(3)
    round_four(1)

    head_dim = D // HEADS
    factor = 1.0 / math.sqrt(head_dim)
    arrived = abuf.at[sizes(63)]
    pltpu.make_async_copy(arrived, arrived, a_recv).wait()
    rows = abuf[...].astype(F32)
    xr = rows[:, 0:2, :].reshape(128, D)
    g = rows[:, 2:4, :].reshape(128, D)
    sums[4:5, :] = jnp.sum(g, axis=0, keepdims=True)
    g_s[...] = g.astype(BF16)
    mean = jnp.mean(xr, axis=-1, keepdims=True)
    centred = xr - mean
    inv_std = lax.rsqrt(jnp.mean(centred * centred, axis=-1, keepdims=True) + EPS)
    normal = centred * inv_std
    gain = gain_ref[...].reshape(1, D)
    normed = (normal * gain).astype(BF16)

    round_four(2)
    round_four(3)
    half = wbuf.at[sizes(8 * D)]
    pltpu.make_async_copy(half, half, d_recv).wait()
    for j in range(9):
        qkv_s[:, CH * j : CH * j + CH] = (
            mm(normed, wbuf[j * D : j * D + D, :], NN) + bias_ref[CH * j : CH * j + CH].reshape(1, CH)
        ).astype(BF16)
    acc = None
    for j in range(3):
        part = mm(g_s[:, CH * j : CH * j + CH], wbuf[(9 + j) * D : (10 + j) * D, :], NT)
        acc = part if acc is None else acc + part
    ga_s[...] = acc.astype(BF16)
    ri = lax.broadcasted_iota(jnp.int32, (128, 128), 0)
    ci = lax.broadcasted_iota(jnp.int32, (128, 128), 1)
    mask = (ri & 1) == (ci & 1)
    for h in range(HEADS):
        lo, hi = h * head_dim, (h + 1) * head_dim
        qh, kh = qkv_s[:, lo:hi], qkv_s[:, D + lo : D + hi]
        gq, gk, gv = grads_of(
            softmax_of(qh, kh, factor, mask), qh, kh, qkv_s[:, 2 * D + lo : 2 * D + hi],
            ga_s[:, lo:hi], factor,
        )
        dq_s[:, lo:hi] = gq
        dq_s[:, D + lo : D + hi] = gk
        dq_s[:, 2 * D + lo : 2 * D + hi] = gv
    acc = None
    for j in range(9):
        part = mm(dq_s[:, CH * j : CH * j + CH], wbuf[j * D : j * D + D, :], NT)
        acc = part if acc is None else acc + part
    grad_normed = acc
    hat = grad_normed * gain
    branch = inv_std * (
        hat
        - jnp.mean(hat, axis=-1, keepdims=True)
        - normal * jnp.mean(hat * normal, axis=-1, keepdims=True)
    )
    bsrc[...] = branch.reshape(64, 2, D).astype(BF16)

    for dz in (8, 7, 9, 6, 10, 5, 11, 4, 12, 3, 13, 2, 14, 1, 15):
        zz = (z + dz) % NZ

        def back(i, carry):
            t = ((ylo + i // 2) % 2) * 32 + zz * 2 + (c + i) % 2
            pltpu.make_async_remote_copy(
                bsrc.at[t], brecv.at[s], b_send, b_recv,
                device_id={"clip": q, "seq": t}, device_id_type=MESH,
            ).start()
            return carry

        lax.fori_loop(0, 4, back, 0)
    for yl, cc in ((1 - ylo, c), (1 - ylo, 1 - c), (ylo, 1 - c)):
        t = yl * 32 + z * 2 + cc
        pltpu.make_async_remote_copy(
            bsrc.at[t], brecv.at[s], b_send, b_recv,
            device_id={"clip": q, "seq": t}, device_id_type=MESH,
        ).start()
    brecv[s] = bsrc[s]

    sums[0:1, :] = jnp.sum(grad_normed * normal, axis=0, keepdims=True)
    for j in range(3):
        sums[1 + j : 2 + j, :] = jnp.sum(
            dq_s[:, D * j : D * j + D].astype(F32), axis=0, keepdims=True
        )
    for h in range(HEADS):
        lo, hi = h * head_dim, (h + 1) * head_dim
        sw_s[h] = softmax_of(sq_ref[:, lo:hi], sq_ref[:, D + lo : D + hi], factor, None)

    pltpu.make_async_copy(brecv.at[pl.ds(0, 63)], brecv.at[pl.ds(0, 63)], b_recv).wait()
    resid = (g_ref[...].astype(F32) + brecv[...].astype(F32).reshape(128, D)).astype(BF16)
    resid_ref[...] = resid
    sums[8:9, :] = jnp.sum(resid.astype(F32), axis=0, keepdims=True)
    acc = None
    for j in range(3):
        part = mm(resid_ref[:, CH * j : CH * j + CH], wbuf[(12 + j) * D : (13 + j) * D, :], NT)
        acc = part if acc is None else acc + part
    ga_s[...] = acc.astype(BF16)
    for h in range(HEADS):
        lo, hi = h * head_dim, (h + 1) * head_dim
        gq, gk, gv = grads_of(
            sw_s[h], sq_ref[:, lo:hi], sq_ref[:, D + lo : D + hi],
            sq_ref[:, 2 * D + lo : 2 * D + hi], ga_s[:, lo:hi], factor,
        )
        dqkv_ref[:, lo:hi] = gq
        dqkv_ref[:, D + lo : D + hi] = gk
        dqkv_ref[:, 2 * D + lo : 2 * D + hi] = gv
    for j in range(3):
        sums[5 + j : 6 + j, :] = jnp.sum(
            dqkv_ref[:, D * j : D * j + D].astype(F32), axis=0, keepdims=True
        )

    pair = pltpu.make_async_remote_copy(
        sums, mate, m_send, m_recv, device_id=sib, device_id_type=MESH
    )
    pair.start()
    pair.wait_recv()
    both = sums[...] + mate[...]
    mine = jnp.where(c == 0, both[0:8], jnp.concatenate([both[5:9], both[9:13]], axis=0))
    for k in range(NZ):
        for yl in range(2):
            lo = yl * 576 + 36 * k
            slab[k, :, 36 * yl : 36 * yl + 36] = mine[:, lo : lo + 36]

    def xy_peer(i):
        return (x + i // 4) % 4, (y + i % 4) % 4

    def zsend(i, carry):
        k = (z + i) % NZ
        pltpu.make_async_remote_copy(
            slab.at[k], zin.at[z], z_send, z_recv, device_id=dev(x, y, k, c), device_id_type=MESH
        ).start()
        return carry

    def psend(i, carry):
        pltpu.make_async_remote_copy(
            zin.at[NZ], pin.at[x * 4 + y], q_send, q_recv,
            device_id=dev(*xy_peer(i), z, c), device_id_type=MESH,
        ).start()
        return carry

    lax.fori_loop(1, 16, zsend, 0)
    zin[z] = slab[z]
    pltpu.make_async_copy(zin.at[pl.ds(0, 15)], zin.at[pl.ds(0, 15)], z_recv).wait()
    zsum = jnp.sum(zin[0:NZ], axis=0)
    zin[NZ] = zsum
    lax.fori_loop(1, 16, psend, 0)
    pin[x * 4 + y] = zsum
    pltpu.make_async_copy(pin.at[pl.ds(0, 15)], pin.at[pl.ds(0, 15)], q_recv).wait()
    psum = jnp.sum(pin[...], axis=0)
    fin[c] = psum
    last = pltpu.make_async_remote_copy(
        fin.at[c], fin.at[c], f_send, f_recv, device_id=sib, device_id_type=MESH
    )
    last.start()
    pltpu.make_async_remote_copy(
        fin.at[c], fin.at[1 - c], f_send, f_recv, device_id=sib, device_id_type=MESH
    ).wait_recv()
    total = jnp.concatenate([fin[0, 0:5], fin[1, 0:4]], axis=0)
    part = ylo * 2 + c
    pick = total[:, 0:18]
    for k in range(1, 4):
        pick = jnp.where(part == k, total[:, 18 * k : 18 * k + 18], pick)
    tot_ref[...] = pick * (1.0 / math.sqrt(tokens))

    swap.wait_send()
    pair.wait_send()
    last.wait_send()

    def drain(ref, rows, sem):
        view = ref.at[sizes(rows)]
        pltpu.make_async_copy(view, view, sem).wait()

    drain(asrc, 63, a_send)
    drain(bsrc, 63, b_send)
    drain(zin, 15, z_send)
    drain(pin, 15, q_send)
    drain(wbuf, 60 * UNIT, p_send)
    drain(wbuf, 8 * D, d_send)
    drain(zbuf, 15, zg_send)


def block(ws, x, g, sq, gain, bias, tokens):
    vm = pl.BlockSpec(memory_space=pltpu.VMEM)
    dma = pltpu.SemaphoreType.DMA
    return pl.pallas_call(
        functools.partial(block_kernel, tokens),
        out_shape=(
            jax.ShapeDtypeStruct((128, D), BF16),
            jax.ShapeDtypeStruct((128, 3 * D), BF16),
            jax.ShapeDtypeStruct((9, D // 64), F32),
        ),
        in_specs=[pl.BlockSpec(memory_space=pl.ANY)] + [vm] * 5,
        out_specs=(vm, vm, vm),
        scratch_shapes=[
            pltpu.VMEM((NZ, 2, 54, 128), BF16),
            pltpu.VMEM((NCH * D, CH), BF16),
            pltpu.VMEM((64, 4, D), BF16),
            pltpu.VMEM((64, 4, D), BF16),
            pltpu.VMEM((128, 3 * D), BF16),
            pltpu.VMEM((128, D), BF16),
            pltpu.VMEM((128, D), BF16),
            pltpu.VMEM((128, 3 * D), BF16),
            pltpu.VMEM((HEADS, 128, 128), F32),
            pltpu.VMEM((64, 2, D), BF16),
            pltpu.VMEM((64, 2, D), BF16),
            pltpu.VMEM((16, D), F32),
            pltpu.VMEM((16, D), F32),
            pltpu.VMEM((NZ, 8, 128), F32),
            pltpu.VMEM((NZ + 1, 8, 128), F32),
            pltpu.VMEM((16, 8, 128), F32),
            pltpu.VMEM((2, 8, 128), F32),
            dma, dma, dma, dma, dma((NZ,)), dma, dma, dma, dma((128,)), dma, dma,
            dma, dma, dma, dma, dma, dma, dma, dma, dma, dma,
        ],
        compiler_params=pltpu.CompilerParams(
            collective_id=0, has_side_effects=True, vmem_limit_bytes=56 << 20
        ),
        name="block",
    )(ws, x, g, sq, gain, bias)


def hand_kernel(resid_ref, dqkv_ref, tot_ref, gsum_ref, resid_out, dqkv_out, tot_out):
    resid_out[...] = resid_ref[...]
    dqkv_out[...] = dqkv_ref[...]
    tot_out[...] = gsum_ref[...] + tot_ref[...]


def hand_over(resid, dqkv, tot, gsum):
    vm = pl.BlockSpec(memory_space=pltpu.VMEM)
    return pl.pallas_call(
        hand_kernel,
        out_shape=(
            jax.ShapeDtypeStruct(resid.shape, BF16),
            jax.ShapeDtypeStruct(dqkv.shape, BF16),
            jax.ShapeDtypeStruct(tot.shape, F32),
        ),
        in_specs=[vm] * 4,
        out_specs=(vm, vm, vm),
        name="hand_over",
    )(resid, dqkv, tot, gsum)


def per_device(
    block_input, out_grad, spatial_qkv, norm_gain, qkv_weight, qkv_bias, out_weight,
    spatial_out_weight, grad_sums,
):
    rows = qkv_weight.shape[0]
    pad = jnp.zeros((rows, CH), BF16)
    w = jnp.concatenate([qkv_weight, out_weight, spatial_out_weight, pad], axis=1)
    ws = w.reshape(rows, NCH, 3, 128).transpose(1, 2, 0, 3).reshape(NCH, 3 * rows, 128)
    tokens = 128 * lax.axis_size("seq") * lax.axis_size("clip")
    resid, sgrad, totals = block(
        ws, block_input.reshape(128, D), out_grad.reshape(128, D), spatial_qkv.reshape(128, 3 * D),
        norm_gain, qkv_bias, tokens,
    )
    resid, sgrad, totals = hand_over(resid, sgrad, totals, grad_sums)
    return resid.reshape(1, 1, 128, D), sgrad.reshape(1, 1, 128, 3 * D), totals


def solution(mesh):
    in_specs = (
        P("clip", "seq", None, None),
        P("clip", "seq", None, None),
        P("clip", "seq", None, None),
        P(),
        P("seq", None),
        P(),
        P("seq", None),
        P("seq", None),
        P(None, "seq"),
    )
    out_specs = (P("clip", "seq", None, None), P("clip", "seq", None, None), P(None, "seq"))
    return jax.shard_map(
        per_device, mesh=mesh, in_specs=in_specs, out_specs=out_specs, check_vma=False
    )
```
